32 devices in a mesh: px: 8 (over y, x, core), py: 4 (over z).
Axes of the slice: x: 2, y: 2, z: 4, core: 2. Of those that a mesh axis runs over, the one named last changes fastest.
Arguments:
- cell_ids: int32 [8, 2560, 128], P('px', 'py'), may hold values from 0 to 262143, as said below
- offset_x: bfloat16 [8, 2560, 128], P('px', 'py'), may hold values from 0 to 1
- offset_y: bfloat16 [8, 2560, 128], P('px', 'py'), may hold values from 0 to 1
- mass: bfloat16 [8, 2560, 128], P('px', 'py'), may hold values from 0.25 to 4
- live: int32 [8, 2560, 128], P('px', 'py'), may hold values from 0 to 1, as said below
- tile_owner: int32 [8, 2560], P('px', 'py'), may hold values from 0 to 7, as said below
- counts: int32 [8, 4, 64], P('px', 'py'), may hold values from 0 to 30720, as said below
Outputs:
- spectrum: float32 [2, 8, 1024, 1024], P(None, None, ('px', 'py'))
- bucket_start: int32 [8, 4, 64], P('px', 'py')
The draws below stay inside these ranges and needn't reach their ends.
Inputs may be any that keep to these rules, and one draw needn't show every extreme that they name: A device's tiles stand in order of bucket, bucket = tile_owner * 8 + plane. One device has at most 240 tiles of one owner; in every draw, in each column of py, one owner has exactly 240 tiles on every device of that column. `cell_ids`: cell = (plane * 128 + row) * 256 + column, with row inside the owner's block of rows and column inside the device's block of columns; all slots of a tile, padded ones too, carry the tile's plane. In a tile the live particles come first; only the last tile of a bucket on a device has padded slots. counts[i, j, b] is the number of live particles in the tiles of bucket b on device (i, j); in every draw some bucket of every device holds 30720.
All inputs are finite; a program needn't handle non-finite values.
Results may differ from the reference program's by a relative error of at most 0.0003.
The reference program's roundings to bfloat16 on the way (of `weights`, `weight_x` and `weight_y`) count: a program that leaves them out, or rounds other values in their place, can miss the bound.
Values may be sent and summed in bfloat16 or wider, within the bound.
A program may use at most 192 MiB of HBM per device.

```python
import math
import jax
import jax.numpy as jnp
from jax import lax

NX = 1024
NY = 1024
PLANES = 8
TILE = 128
TILES_DEV = 640
RX = 128
RY = 256
CAP = 240
BUCKETS = 64
N_PX = 8
N_PY = 4


def tile_layout(key):
    base_key = jax.random.fold_in(key, 7001)
    key_hot, key_jitter, key_plane, key_fill = jax.random.split(base_key, 4)
    hot_owner = jax.random.randint(key_hot, (N_PY,), 0, N_PX)
    owner_ids = jnp.arange(N_PX, dtype=jnp.int32)
    is_hot = jnp.broadcast_to(owner_ids[None, None, :] == hot_owner[None, :, None], (N_PX, N_PY, N_PX))
    jitter = jax.random.randint(key_jitter, (N_PX, N_PY, N_PX), 1, 3)
    weights = jnp.where(is_hot, 0, (N_PX - 1 + 2 * owner_ids)[None, None, :] * jitter)
    remain = TILES_DEV - CAP
    shares = remain * weights // jnp.sum(weights, axis=-1, keepdims=True)
    leftover = remain - jnp.sum(shares, axis=-1, keepdims=True)
    order_rank = jnp.cumsum(jnp.where(is_hot, 0, 1), axis=-1) - 1
    shares = shares + jnp.where(jnp.logical_not(is_hot) & (order_rank < leftover), 1, 0)
    run_length = jnp.where(is_hot, CAP, shares)
    run_end = jnp.cumsum(run_length, axis=-1)
    tile_index = jnp.arange(TILES_DEV, dtype=jnp.int32)
    owner_of = jnp.sum((tile_index[None, None, :, None] >= run_end[:, :, None, :]).astype(jnp.int32), axis=-1)
    hot_of = jnp.broadcast_to(hot_owner[None, :, None], (N_PX, N_PY, TILES_DEV))
    tile_is_hot = owner_of == hot_of
    plane_draw = jax.random.randint(key_plane, (N_PX, N_PY, TILES_DEV), 0, PLANES)
    plane_draw = jnp.where(tile_is_hot, 0, plane_draw)
    sort_key = jnp.sort((owner_of * PLANES + plane_draw).astype(jnp.int32), axis=-1)
    closing = jnp.full((N_PX, N_PY, 1), -1, jnp.int32)
    is_last = sort_key != jnp.concatenate([sort_key[..., 1:], closing], axis=-1)
    sorted_hot = sort_key // PLANES == hot_of
    fill_count = jax.random.randint(key_fill, (N_PX, N_PY, TILES_DEV), 1, TILE + 1)
    live_count = jnp.where(is_last & jnp.logical_not(sorted_hot), fill_count, TILE)
    return (sort_key, live_count)


def bucket_tally(keys_row, live_row):
    return jax.ops.segment_sum(live_row, keys_row, num_segments=BUCKETS)


def draw_tile_owner(key, part):
    sort_key, live_count = tile_layout(key)
    return (sort_key // PLANES).reshape(N_PX, N_PY * TILES_DEV).astype(jnp.int32)


def draw_live(key, part):
    sort_key, live_count = tile_layout(key)
    slot_index = jnp.arange(TILE, dtype=jnp.int32)
    flags = (slot_index[None, None, None, :] < live_count[..., None]).astype(jnp.int32)
    return flags.reshape(N_PX, N_PY * TILES_DEV, TILE)


def draw_counts(key, part):
    sort_key, live_count = tile_layout(key)
    bucket_sums = jax.vmap(bucket_tally)(sort_key.reshape(-1, TILES_DEV), live_count.reshape(-1, TILES_DEV))
    return bucket_sums.reshape(N_PX, N_PY, BUCKETS).astype(jnp.int32)


def draw_cell_ids(key, part):
    sort_key, live_count = tile_layout(key)
    plane_ids = sort_key % PLANES
    key_x, key_y = jax.random.split(jax.random.fold_in(key, 7002))
    local_x = jax.random.randint(key_x, (N_PX, N_PY, TILES_DEV, TILE), 0, RX)
    local_y = jax.random.randint(key_y, (N_PX, N_PY, TILES_DEV, TILE), 0, RY)
    cells_all = (plane_ids[..., None] * RX + local_x) * RY + local_y
    return cells_all.reshape(N_PX, N_PY * TILES_DEV, TILE).astype(jnp.int32)


def steps_of(stream_key, shape, cuts, low, top_value):
    def one(dim, shards_of):
        steps = jax.random.uniform(jax.random.fold_in(jax.random.fold_in(stream_key, 6), dim), (shards_of,), jnp.float32, low / len(cuts), top_value / len(cuts))
        return jnp.repeat(jnp.exp(steps), shape[dim] // shards_of).reshape((-1,) + (1,) * (len(shape) - dim - 1))

    factor_of = one(*cuts[0])
    for cut in cuts[1:]:
        factor_of = factor_of * one(*cut)
    return factor_of


def setup_inputs(seed: int = 0) -> dict:
    keys = jax.random.split(jax.random.key(seed), 8)
    return {
        "cell_ids": draw_cell_ids(jax.random.fold_in(keys[7], 71), 0),
        "offset_x": jnp.clip(1.0 * jax.random.uniform(keys[1], (N_PX, N_PY * TILES_DEV, TILE), jnp.float32) ** steps_of(keys[1], (N_PX, N_PY * TILES_DEV, TILE), ((0, 8), (1, 4)), -0.2, 0.2), 0.0, 1.0).astype(jnp.bfloat16),
        "offset_y": jnp.clip(1.0 * jax.random.uniform(keys[2], (N_PX, N_PY * TILES_DEV, TILE), jnp.float32) ** steps_of(keys[2], (N_PX, N_PY * TILES_DEV, TILE), ((0, 8), (1, 4)), -0.2, 0.2), 0.0, 1.0).astype(jnp.bfloat16),
        "mass": jnp.clip(jnp.exp(math.log(4.0) - 2.7725887 * jax.random.uniform(keys[3], (N_PX, N_PY * TILES_DEV, TILE), jnp.float32) ** steps_of(keys[3], (N_PX, N_PY * TILES_DEV, TILE), ((0, 8), (1, 4)), -0.2, 0.2)), 0.25, 4.0).astype(jnp.bfloat16),
        "live": draw_live(jax.random.fold_in(keys[7], 71), 0),
        "tile_owner": draw_tile_owner(jax.random.fold_in(keys[7], 71), 0),
        "counts": draw_counts(jax.random.fold_in(keys[7], 71), 0),
    }


BETA = 18.4

def kernel(spread_at):
    return jnp.exp(BETA * (jnp.sqrt(1.0 - spread_at * spread_at) - 1.0))

def reference(cell_ids, offset_x, offset_y, mass, live, tile_owner, counts):
    tile_shape = (N_PX, N_PY, TILES_DEV, TILE)
    tile_cells = cell_ids.reshape(tile_shape)
    frac_x = offset_x.reshape(tile_shape).astype(jnp.float32)
    frac_y = offset_y.reshape(tile_shape).astype(jnp.float32)
    masses = jnp.where(live == 1, mass, jnp.zeros_like(mass)).reshape(tile_shape).astype(jnp.float32)
    owners = tile_owner.reshape(N_PX, N_PY, TILES_DEV)
    offset_steps = jnp.arange(-3, 5, dtype=jnp.int32)
    step_values = offset_steps.astype(jnp.float32)
    column_base = (jnp.arange(N_PY, dtype=jnp.int32) * RY)[:, None, None]

    def deposit_rows(density_flat, source_rows):
        row_cells, row_x, row_y, row_mass, row_owner = source_rows
        local_y = row_cells % RY
        local_x = row_cells // RY % RX
        plane_ids = row_cells // (RY * RX)
        global_x = row_owner[:, :, None] * RX + local_x
        global_y = column_base + local_y
        weight_x = kernel((step_values - row_x[..., None]) / 4.0).astype(jnp.bfloat16)
        weight_y = (kernel((step_values - row_y[..., None]) / 4.0) * row_mass[..., None]).astype(jnp.bfloat16)
        weight_x, weight_y = lax.optimization_barrier((weight_x, weight_y))
        values = weight_x.astype(jnp.float32)[..., :, None] * weight_y.astype(jnp.float32)[..., None, :]
        rows_at = (global_x[..., None] + offset_steps) % NX
        columns_at = (global_y[..., None] + offset_steps) % NY
        flat_index = (plane_ids[..., None, None] * NX + rows_at[..., :, None]) * NY + columns_at[..., None, :]
        return (density_flat.at[flat_index.reshape(-1)].add(values.reshape(-1)), None)
    initial = jnp.zeros((PLANES * NX * NY,), jnp.float32)
    density_flat = lax.scan(deposit_rows, initial, (tile_cells, frac_x, frac_y, masses, owners))[0]
    density = density_flat.reshape(PLANES, NX, NY)
    mean_density = jnp.sum(density) / (PLANES * NX * NY)
    contrast = density / mean_density - 1.0
    transform = jnp.fft.fft2(contrast, axes=(1, 2)) / math.sqrt(NX * NY)
    transform = jnp.transpose(transform, (0, 2, 1))
    spectrum = jnp.stack([jnp.real(transform), jnp.imag(transform)]).astype(jnp.float32)
    column_totals = lax.optimization_barrier(jnp.sum(counts, axis=0))
    preceding = jnp.cumsum(column_totals, axis=-1) - column_totals
    earlier = jnp.cumsum(counts, axis=0) - counts
    bucket_start = (preceding[None] + earlier).astype(jnp.int32)
    return (spectrum, bucket_start)
```

```python
import functools
import math

import jax
import jax.numpy as jnp
import numpy as np
from jax import lax
from jax.experimental import pallas as pl
from jax.experimental.pallas import tpu as pltpu
from jax.sharding import PartitionSpec as P

NX = 1024
NY = 1024
PLANES = 8
BETA = 18.4
LANES = 128
GROUP = 4
UNROLL = 8
EAGER = 3
RATE = BETA / math.log(2.0)


def tap_blocks(start, fraction, scaling, rows):
    depth = (rows - start + 3) & 7
    z = ((depth - 3).astype(jnp.float32) - fraction) * 0.25
    u = jnp.maximum(1.0 - z * z, 0.0)
    taps = jnp.exp2(u * lax.rsqrt(jnp.maximum(u, 1e-30)) * RATE - RATE)
    if scaling is not None:
        taps = taps * scaling
    at = start - 3 + depth
    odd = (at & 8) != 0
    zero = jnp.zeros_like(taps)
    both = jnp.concatenate(
        [jnp.where(odd, zero, taps), jnp.where(odd, taps, zero)], axis=0
    ).astype(jnp.bfloat16)
    return both, at >> 4


def placed_blocks(taps, block, count):
    block = jnp.where(block < 0, count, block)
    block = jnp.concatenate([block, block], axis=0).astype(jnp.int16)
    none = jnp.zeros_like(taps)
    return [jnp.where(block == k, taps, none) for k in range(count + 1)]


def spread_kernel(row_count, col_count, bucket_count, starts_ref, cell_ref, owner_ref, fx_ref, fy_ref,
                  mass_ref, live_ref, out_ref, rim_ref, x_ref, y_ref, w_ref, c_ref, item_ref):
    tiles = cell_ref.shape[0]
    col_blocks = col_count // 16
    lane_tiles = NX // LANES
    owners_tile = LANES // row_count if row_count < LANES else 1
    height = col_count + 16
    rows = lax.broadcasted_iota(jnp.int32, (8, LANES), 0)
    spare = pl.ds(tiles, 8)
    x_ref[pl.ds(0, tiles), :] = fx_ref[...].astype(jnp.float32)
    y_ref[pl.ds(0, tiles), :] = fy_ref[...].astype(jnp.float32)
    mass = mass_ref[...].astype(jnp.float32)
    w_ref[pl.ds(0, tiles), :] = jnp.where(live_ref[...] == 1, mass, jnp.zeros_like(mass))
    c_ref[pl.ds(0, tiles), :] = cell_ref[...]
    for ref in (x_ref, y_ref, w_ref, c_ref):
        ref[spare, :] = jnp.zeros((8, LANES), ref.dtype)
    out_ref[...] = jnp.zeros_like(out_ref)
    rim_ref[...] = jnp.zeros_like(rim_ref)

    def of_bucket(b, at):
        begin = starts_ref[b]
        count = (starts_ref[b + 1] - begin + GROUP - 1) // GROUP
        word = b * 65536 + begin
        for c in range(EAGER):
            item_ref[at + c] = word + c * GROUP

        @pl.when(count > EAGER)
        def _():
            def one(c, _):
                item_ref[at + c] = word + c * GROUP
                return 0

            lax.fori_loop(EAGER, count, one, 0)

        return at + count

    items = lax.fori_loop(0, bucket_count, of_bucket, 0)
    for k in range(UNROLL):
        item_ref[items + k] = (bucket_count - 1) * 65536 + tiles

    def product(k):
        begin = item_ref[k] & 65535
        bucket = lax.shift_right_logical(item_ref[k], 16)
        end = starts_ref[bucket + 1]
        shift = bucket // PLANES % owners_tile * row_count
        wxs, wys = [], []
        for g in range(GROUP):
            t = begin + g
            at = pl.ds(t, 1)
            scale = jnp.where(t < end, 1.0, 0.0)
            cell = jnp.broadcast_to(c_ref[at, :], (8, LANES))
            lx = lax.shift_right_logical(cell, col_count.bit_length() - 1) & (row_count - 1)
            if owners_tile > 1:
                lx = lx + shift
            taps, block = tap_blocks(lx, x_ref[at, :], None, rows)
            wxs.append(jnp.concatenate(placed_blocks(taps, block, LANES // 16), axis=0))
            taps, block = tap_blocks(cell & (col_count - 1), y_ref[at, :], w_ref[at, :] * scale, rows)
            wys.append(jnp.concatenate(placed_blocks(taps, block, col_blocks), axis=0))
        return lax.dot_general(
            jnp.concatenate(wys, axis=1), jnp.concatenate(wxs, axis=1),
            (((1,), (1,)), ((), ())), preferred_element_type=jnp.float32
        )

    def some(i, _):
        results = [product(i * UNROLL + u) for u in range(UNROLL)]
        for u, result in enumerate(results):
            b = lax.shift_right_logical(item_ref[i * UNROLL + u], 16)
            plane = b % PLANES
            tile = (b // PLANES * row_count) // LANES
            out_ref[plane, tile] += result[:, :LANES]
            rim_ref[plane, tile] += jnp.concatenate(
                [result[:, LANES:], jnp.zeros((height, LANES - 16), jnp.float32)], axis=1
            )
        return 0

    lax.fori_loop(0, (items + UNROLL - 1) // UNROLL, some, 0)

    lane = lax.broadcasted_iota(jnp.int32, (8, LANES), 1)

    def close(i, _):
        plane = i // 2
        for k in range(lane_tiles // 2):
            tile = i % 2 * (lane_tiles // 2) + k
            low = (tile + lane_tiles - 1) % lane_tiles
            high = (tile + 1) % lane_tiles
            for r in range(0, height, 8):
                at = pl.ds(r, 8)
                left = jnp.where(lane < 8, rim_ref[plane, low, at, :], 0.0)
                right = jnp.where(lane < 8, 0.0, rim_ref[plane, high, at, :])
                out_ref[plane, tile, at, :] += left + pltpu.roll(right, LANES - 16, 1)
        return 0

    lax.fori_loop(0, 2 * PLANES, close, 0)


def spread(starts, cells, owners, fx, fy, mass, live, row_count, col_count):
    height = col_count + 16
    bucket_count = starts.shape[0] - 1
    tiles = cells.shape[0]
    vmem = pl.BlockSpec(memory_space=pltpu.VMEM)
    smem = pl.BlockSpec(memory_space=pltpu.SMEM)
    width = LANES + 16
    depth = GROUP * LANES
    return pl.pallas_call(
        functools.partial(spread_kernel, row_count, col_count, bucket_count),
        out_shape=jax.ShapeDtypeStruct((PLANES, NX // LANES, height, LANES), jnp.float32),
        in_specs=[smem, vmem, smem] + [vmem] * 4,
        out_specs=vmem,
        scratch_shapes=[
            pltpu.VMEM((PLANES, NX // LANES, height, LANES), jnp.float32),
            pltpu.VMEM((tiles + 8, LANES), jnp.float32),
            pltpu.VMEM((tiles + 8, LANES), jnp.float32),
            pltpu.VMEM((tiles + 8, LANES), jnp.float32),
            pltpu.VMEM((tiles + 8, LANES), jnp.int32),
            pltpu.SMEM((-(-tiles // GROUP) + bucket_count + UNROLL + EAGER,), jnp.int32),
        ],
        compiler_params=pltpu.CompilerParams(vmem_limit_bytes=40 * 1024 * 1024),
        name="spread",
    )(starts, cells, owners, fx, fy, mass, live)


def split(value):
    high = lax.reduce_precision(value, 8, 7)
    return high.astype(jnp.bfloat16), (value - high).astype(jnp.bfloat16)


def dft_parts():
    n = np.arange(NX)
    k = np.arange(32)
    coarse = 2.0 * np.pi / NX * ((32 * k[:, None] * n[None, :]) % NX)
    fine = 2.0 * np.pi / NX * ((k[:, None] * n[None, :]) % NX)
    return tuple(jnp.asarray(f(a), jnp.float32) for a in (coarse, fine) for f in (np.cos, np.sin))


def dft_tables():
    cc, cs, fc, fs = lax.optimization_barrier(dft_parts())
    cc, cs = cc[:, None, :], cs[:, None, :]
    fc, fs = fc[None, :, :], fs[None, :, :]
    cosine = (cc * fc - cs * fs).reshape(NX, NX)
    sine = (cs * fc + cc * fs).reshape(NX, NX)
    return split(cosine) + split(sine)


def dot(a, b):
    return jnp.dot(a, b, preferred_element_type=jnp.float32)


def power_of(top):
    return jnp.clip(jnp.floor(jnp.log2(jnp.maximum(top, 1e-30))) + 1.0, -90.0, 90.0).astype(jnp.int32)


def scale_of(power):
    return jnp.exp2((power - 15).astype(jnp.float32))


def coded_as(value, power):
    steps = jnp.round(value * jnp.exp2((15 - power).astype(jnp.float32)))
    return jnp.clip(steps, -32767.0, 32767.0).astype(jnp.int16)


def coded_rows(value, spare):
    power = power_of(jnp.max(jnp.abs(value), axis=-2, keepdims=True))
    row = lax.broadcasted_iota(jnp.int32, value.shape, value.ndim - 2)
    return jnp.where(row == spare, power.astype(jnp.int16), coded_as(value, power))


def plain_rows(coded, spare):
    power = lax.slice_in_dim(coded, spare, spare + 1, axis=coded.ndim - 2).astype(jnp.int32)
    row = lax.broadcasted_iota(jnp.int32, coded.shape, coded.ndim - 2)
    return jnp.where(row == spare, 0.0, coded.astype(jnp.float32) * scale_of(power))


def digits(value, width):
    power = power_of(value)
    scaled = value * jnp.exp2((14 - power).astype(jnp.float32))
    high = jnp.clip(jnp.floor(scaled), 0.0, 32767.0)
    low = jnp.clip(jnp.floor((scaled - high) * 16384.0), 0.0, 16384.0)
    lane = lax.broadcasted_iota(jnp.int32, (1, width), 1)
    rest = jnp.where(lane == 1, high, low).astype(jnp.int32)
    return jnp.where(lane == 0, power, rest)


def number(row):
    value = row[..., 1].astype(jnp.float32) + row[..., 2].astype(jnp.float32) / 16384.0
    return value * jnp.exp2((row[..., 0] - 14).astype(jnp.float32))


def scaled(out, total):
    py_count = lax.axis_size("py")
    ky_part = out.shape[2]
    norm = 1.0 / math.sqrt(NX * NY)
    index = lax.axis_index("px") * py_count + lax.axis_index("py")
    shape = (2, 1, ky_part, NX)
    at_zero = (
        (lax.broadcasted_iota(jnp.int32, shape, 0) == 0)
        & (lax.broadcasted_iota(jnp.int32, shape, 2) + index == 0)
        & (lax.broadcasted_iota(jnp.int32, shape, 3) == 0)
    )
    return out * (PLANES * NX * NY * norm / total) - jnp.where(at_zero, NX * NY * norm, 0.0)


def code_power(top):
    return jnp.clip(jnp.floor(jnp.log2(jnp.maximum(top, 1e-30))) + 1.0, -90.0, 90.0)


def code_block(read, store, row_groups, spare):
    top = None
    for r in range(row_groups):
        here = jnp.abs(read(r))
        top = here if top is None else jnp.maximum(top, here)
    power = code_power(jnp.max(top, axis=0, keepdims=True))
    factor = jnp.exp2(15.0 - power)
    for r in range(row_groups):
        steps = jnp.clip(jnp.round(read(r) * factor), -32767.0, 32767.0)
        if r == row_groups - 1 and spare is not None:
            row = lax.broadcasted_iota(jnp.int32, steps.shape, 0)
            steps = jnp.where(row == spare, power, steps)
        store(r, steps.astype(jnp.int32).astype(jnp.int16))
    return power


def exchange_kernel(px_count, py_count, grid_ref, counts_ref, coarse_c_ref, coarse_s_ref, fine_c_ref,
                    fine_s_ref, out_ref, total_ref, starts_ref,
                    pair_ref, own_ref, code_ref, got_ref, zcode_ref, zgot_ref, data_ref, dhl_ref,
                    chi_ref, clo_ref, shi_ref, slo_ref, fcode_ref, fgot_ref, lhs_ref, line_ref,
                    pair_send, pair_recv, code_send, code_recv, z_send, z_recv, f_send, f_recv):
    px = lax.axis_index("px")
    py = lax.axis_index("py")
    core = px % 2
    chip = px // 2
    chips = px_count // 2
    other = px + 1 - 2 * core
    blocks, tiles, height, _ = grid_ref.shape
    part = tiles // py_count
    col_count = height - 16
    groups = height // 16
    spare = 8
    width = part * LANES
    devices = px_count * py_count
    ky_part = NY // devices

    barrier = pltpu.get_barrier_semaphore()
    for e in range(2):
        for s in range(chips):
            for m in range(py_count):
                if e + s + m > 0:
                    to = ((chip + s) % chips * 2 + (core + e) % 2, (py + m) % py_count)
                    pl.semaphore_signal(barrier, inc=1, device_id=to, device_id_type=pl.DeviceIdType.MESH)
    pl.semaphore_wait(barrier, devices - 1)

    order = [(m, s) for m in range(py_count - 1, -1, -1) for s in range(chips - 1, -1, -1)]

    def pair_copy(m, s):
        q = (py + m) % py_count
        block = (chip + s) % chips * 2
        return pltpu.make_async_remote_copy(
            src_ref=grid_ref.at[block + 1 - core, pl.ds(q * part, part)],
            dst_ref=pair_ref.at[m, s],
            send_sem=pair_send.at[m, s],
            recv_sem=pair_recv.at[m, s],
            device_id=(other, py),
            device_id_type=pl.DeviceIdType.MESH,
        )

    def code_copy(m, s):
        return pltpu.make_async_remote_copy(
            src_ref=code_ref.at[m, s],
            dst_ref=got_ref.at[m, s],
            send_sem=code_send.at[m, s],
            recv_sem=code_recv.at[m, s],
            device_id=((chip + s) % chips * 2 + core, py),
            device_id_type=pl.DeviceIdType.MESH,
        )

    def z_copy(m):
        return pltpu.make_async_remote_copy(
            src_ref=zcode_ref.at[m],
            dst_ref=zgot_ref.at[m],
            send_sem=z_send.at[m],
            recv_sem=z_recv.at[m],
            device_id=(px, (py + m) % py_count),
            device_id_type=pl.DeviceIdType.MESH,
        )

    def f_copy(s, e, m):
        return pltpu.make_async_remote_copy(
            src_ref=fcode_ref.at[s, e, m],
            dst_ref=fgot_ref.at[m, s, e],
            send_sem=f_send.at[s, e, m],
            recv_sem=f_recv.at[s, e, m],
            device_id=((chip + s) % chips * 2 + (core + e) % 2, (py + m) % py_count),
            device_id_type=pl.DeviceIdType.MESH,
        )

    for m, s in order:
        pair_copy(m, s).start()

    for m, s in order:
        pair_copy(m, s).wait_recv()
        q = (py + m) % py_count
        block = (chip + s) % chips * 2 + core

        def add(t, _):
            def summed(r):
                at = pl.ds(r * 16, 16)
                return grid_ref[block, q * part + t, at, :] + pair_ref[m, s, t, at, :]

            if s == 0:
                for r in range(groups):
                    own_ref[m, t, pl.ds(r * 16, 16), :] = summed(r)
            else:
                def keep(r, value):
                    code_ref[m, s, t, pl.ds(r * 16, 16), :] = value

                code_block(summed, keep, groups, spare)
            return 0

        lax.fori_loop(0, part, add, 0)
        if s > 0:
            code_copy(m, s).start()

    def table(a, _):
        at = pl.ds(pl.multiple_of(a * 32, 32), 32)
        cc = coarse_c_ref[pl.ds(a, 1), :]
        cs = coarse_s_ref[pl.ds(a, 1), :]
        fc = fine_c_ref[...]
        fs = fine_s_ref[...]
        for value, high_ref, low_ref in (
            (cc * fc - cs * fs, chi_ref, clo_ref),
            (cs * fc + cc * fs, shi_ref, slo_ref),
        ):
            high = value.astype(jnp.bfloat16)
            high_ref[at, :] = high
            low_ref[at, :] = (value - high.astype(jnp.float32)).astype(jnp.bfloat16)
        return 0

    lax.fori_loop(0, NX // 32, table, 0)

    def scale_from(rows):
        return jnp.exp2(rows[8:9].astype(jnp.float32) - 15.0)

    def plain(ref_at, r):
        return ref_at(r).astype(jnp.int32).astype(jnp.float32)

    row16 = lax.broadcasted_iota(jnp.int32, (16, LANES), 0)
    total = jnp.zeros((16, LANES), jnp.float32)
    for m in range(py_count - 1, -1, -1):
        for s in range(chips - 1, 0, -1):
            code_copy(m, s).wait_recv()

        def gather(t, total):
            scales = [
                jnp.exp2(got_ref[m, s, t, pl.ds(col_count, 16), :].astype(jnp.int32)[8:9].astype(jnp.float32) - 15.0)
                for s in range(1, chips)
            ]

            for r in range(groups):
                at = pl.ds(r * 16, 16)
                value = own_ref[m, t, at, :]
                for s in range(1, chips):
                    term = got_ref[m, s, t, at, :].astype(jnp.int32).astype(jnp.float32) * scales[s - 1]
                    if r == groups - 1:
                        term = jnp.where(row16 == spare, 0.0, term)
                    value = value + term
                own_ref[m, t, at, :] = value
                total = total + value
            if m > 0:
                def keep(r, value):
                    zcode_ref[m, t, pl.ds(r * 16, 16), :] = value

                code_block(lambda r: own_ref[m, t, pl.ds(r * 16, 16), :], keep, groups, spare)
            return total

        total = lax.fori_loop(0, part, gather, total)
        if m > 0:
            z_copy(m).start()

    total = jnp.sum(total)

    def place(m, reader):
        source = (py + py_count - m) % py_count
        for t in range(part):
            cols = pl.ds(t * LANES, LANES)
            for r in range(groups - 1):
                data_ref[source, pl.ds(r * 16, 16), cols] = reader(t, r)

    def rims(m, reader):
        source = (py + py_count - m) % py_count
        after = (source + 1) % py_count
        before = (source + py_count - 1) % py_count
        for t in range(part):
            cols = pl.ds(t * LANES, LANES)
            rim = reader(t, groups - 1)
            low = pl.ds(0, 8)
            high = pl.ds(col_count - 8, 8)
            row = lax.broadcasted_iota(jnp.int32, (8, LANES), 0)
            data_ref[after, low, cols] += jnp.where(row < 4, rim[:8], 0.0)
            data_ref[before, high, cols] += jnp.where(row > 4, rim[8:], 0.0)

    def own_reader(t, r):
        return own_ref[0, t, pl.ds(r * 16, 16), :]

    def z_reader(m):
        def read(t, r):
            scale = jnp.exp2(zgot_ref[m, t, pl.ds(col_count, 16), :].astype(jnp.int32)[8:9].astype(jnp.float32) - 15.0)
            return zgot_ref[m, t, pl.ds(r * 16, 16), :].astype(jnp.int32).astype(jnp.float32) * scale
        return read

    readers = [own_reader] + [z_reader(m) for m in range(1, py_count)]
    place(0, readers[0])
    for m in range(py_count - 1, 0, -1):
        z_copy(m).wait_recv()
        place(m, readers[m])
    for m in range(py_count):
        rims(m, readers[m])
    for j in range(py_count):
        def halves(r, _):
            at = pl.ds(pl.multiple_of(r * 16, 16), 16)
            value = data_ref[j, at, :]
            high = value.astype(jnp.bfloat16)
            to = pl.ds(pl.multiple_of(j * col_count + r * 16, 16), 16)
            dhl_ref[0, to, :] = high
            dhl_ref[1, to, :] = (value - high.astype(jnp.float32)).astype(jnp.bfloat16)
            return 0

        lax.fori_loop(0, col_count // 16, halves, 0)

    power = code_power(total)
    scaled = total * jnp.exp2(14.0 - power)
    first = jnp.clip(jnp.floor(scaled), 0.0, 32767.0)
    second = jnp.clip(jnp.floor((scaled - first) * 16384.0), 0.0, 16384.0)
    row8 = lax.broadcasted_iota(jnp.int32, (8, width), 0)
    lane8 = lax.broadcasted_iota(jnp.int32, (8, width), 1)
    number = jnp.where(lane8 == 0, power, jnp.where(lane8 == 1, first, second))
    side = jnp.where(row8 == 1, number, counts_ref[...].astype(jnp.float32))
    span = 2 * py_count * ky_part

    def transform(s):
        at = pl.ds(pl.multiple_of((chip + s) % chips * span, span), span)
        for high_ref, low_ref, k in ((chi_ref, clo_ref, 0), (shi_ref, slo_ref, 1)):
            value = jnp.dot(high_ref[at, :], dhl_ref[0], preferred_element_type=jnp.float32)
            value += jnp.dot(high_ref[at, :], dhl_ref[1], preferred_element_type=jnp.float32)
            value += jnp.dot(low_ref[at, :], dhl_ref[0], preferred_element_type=jnp.float32)
            line_ref[k] = value if k == 0 else -value
        for e in range(2):
            for m in range(py_count):
                index = (core + e) % 2 * py_count + (py + m) % py_count
                rows = pl.ds(pl.multiple_of(index * ky_part, ky_part), ky_part)
                real = line_ref[0, rows, :]
                imag = line_ref[1, rows, :]
                top = jnp.maximum(jnp.abs(real), jnp.abs(imag))
                power = code_power(jnp.max(top, axis=0, keepdims=True))
                factor = jnp.exp2(15.0 - power)
                for k, value in enumerate((real, imag)):
                    steps = jnp.clip(jnp.round(value * factor), -32767.0, 32767.0)
                    fcode_ref[s, e, m, pl.ds(k * ky_part, ky_part), :] = steps.astype(jnp.int32).astype(jnp.int16)
                rest = jnp.where(row8 == 0, power, side)
                fcode_ref[s, e, m, pl.ds(2 * ky_part, 8), :] = rest.astype(jnp.int32).astype(jnp.int16)

    def send_all(s):
        transform(s)
        for e in range(2):
            for m in range(py_count - 1, -1, -1):
                f_copy(s, e, m).start()
        return 0

    lax.fori_loop(0, chips - 1, lambda k, _: send_all(chips - 1 - k), 0)
    transform(0)
    for e in range(1, -1, -1):
        for m in range(py_count - 1, -1, -1):
            if e + m > 0:
                f_copy(0, e, m).start()

    sum_total = total
    column = jnp.zeros((8, width), jnp.float32)
    before = jnp.zeros((8, width), jnp.float32)
    rows_all = px_count * ky_part
    for m in range(py_count):
        source = (py + py_count - m) % py_count
        for s in range(chips):
            for e in range(2):
                mine = m + s + e == 0
                if not mine:
                    f_copy(s, e, m).wait_recv()
                got = fcode_ref if mine else fgot_ref
                where = (0, 0, 0) if mine else (m, s, e)
                sender = (chip + chips - s) % chips * 2 + (core + e) % 2
                rest = got[where + (pl.ds(2 * ky_part, 8), slice(None))].astype(jnp.int32)
                scale = jnp.exp2(rest[0:1].astype(jnp.float32) - 15.0)
                info = rest.astype(jnp.float32)
                if not mine:
                    digit = info[1:2, :LANES]
                    lane1 = lax.broadcasted_iota(jnp.int32, (1, LANES), 1)
                    body = jnp.sum(jnp.where(lane1 == 1, digit, 0.0) + jnp.where(lane1 == 2, digit * (1.0 / 16384.0), 0.0))
                    bits = jnp.sum(jnp.where(lane1 == 0, digit, 0.0))
                    sum_total = sum_total + body * jnp.exp2(bits - 14.0)
                if m == 0:
                    column = column + info
                    before = before + jnp.where(sender < px, info, 0.0)
                rows = pl.ds(pl.multiple_of(sender * ky_part, ky_part), ky_part)
                rows2 = pl.ds(pl.multiple_of(rows_all + sender * ky_part, ky_part), ky_part)
                real = got[where + (pl.ds(0, ky_part), slice(None))].astype(jnp.int32).astype(jnp.float32) * scale
                imag = got[where + (pl.ds(ky_part, ky_part), slice(None))].astype(jnp.int32).astype(jnp.float32) * scale
                for at, a, b in ((rows, real, imag), (rows2, imag, -real)):
                    for k, value in enumerate((a, b)):
                        high = value.astype(jnp.bfloat16)
                        lhs_ref[0, at, pl.ds(k * width, width)] = high
                        lhs_ref[1, at, pl.ds(k * width, width)] = (value - high.astype(jnp.float32)).astype(jnp.bfloat16)

        xrows = pl.ds(pl.multiple_of(source * width, width), width)

        def columns(n, _):
            cols = pl.ds(pl.multiple_of(n * 256, 256), 256)
            high = lhs_ref[0]
            low = lhs_ref[1]
            ch, cl, sh, sl = (ref[xrows, cols] for ref in (chi_ref, clo_ref, shi_ref, slo_ref))
            hh = jnp.concatenate([ch, sh], axis=0)
            ll = jnp.concatenate([cl, sl], axis=0)
            value = jnp.dot(high, hh, preferred_element_type=jnp.float32)
            value += jnp.dot(low, hh, preferred_element_type=jnp.float32)
            value += jnp.dot(high, ll, preferred_element_type=jnp.float32)
            if m == 0:
                out_ref[:, cols] = value
            else:
                out_ref[:, cols] += value
            return 0

        lax.fori_loop(0, NX // 256, columns, 0)

    total_ref[...] = jnp.full((8, LANES), sum_total, jnp.float32)
    sums = column[2:3]
    lane = lax.broadcasted_iota(jnp.int32, (1, width), 1)
    preceding = sums
    step = 1
    while step < width:
        preceding = preceding + jnp.where(lane >= step, pltpu.roll(preceding, step, 1), 0.0)
        step *= 2
    starts_ref[...] = jnp.broadcast_to(preceding - sums + before[2:3], (8, width)).astype(jnp.int32)

    for m, s in order:
        pair_copy(m, s).wait_send()
        if s > 0:
            code_copy(m, s).wait_send()
    for m in range(1, py_count):
        z_copy(m).wait_send()
    for s in range(chips):
        for e in range(2):
            for m in range(py_count):
                if s + e + m > 0:
                    f_copy(s, e, m).wait_send()


def exchange(grid, counts_row, tables, px_count, py_count):
    blocks, tiles, height, _ = grid.shape
    chips = px_count // 2
    part = tiles // py_count
    width = part * LANES
    col_count = height - 16
    ky_part = NY // (px_count * py_count)
    span = 2 * py_count * ky_part
    rows = px_count * ky_part
    vmem = pl.BlockSpec(memory_space=pltpu.VMEM)
    dma = pltpu.SemaphoreType.DMA
    f32, bf16, s16 = jnp.float32, jnp.bfloat16, jnp.int16
    return pl.pallas_call(
        functools.partial(exchange_kernel, px_count, py_count),
        out_shape=(
            jax.ShapeDtypeStruct((2 * rows, NX), f32),
            jax.ShapeDtypeStruct((8, LANES), f32),
            jax.ShapeDtypeStruct((8, width), jnp.int32),
        ),
        in_specs=[vmem] * 6,
        out_specs=[vmem] * 3,
        scratch_shapes=[
            pltpu.VMEM((py_count, chips, part, height, LANES), f32),
            pltpu.VMEM((py_count, part, height, LANES), f32),
            pltpu.VMEM((py_count, chips, part, height, LANES), s16),
            pltpu.VMEM((py_count, chips, part, height, LANES), s16),
            pltpu.VMEM((py_count, part, height, LANES), s16),
            pltpu.VMEM((py_count, part, height, LANES), s16),
            pltpu.VMEM((py_count, col_count, width), f32),
            pltpu.VMEM((2, NY, width), bf16),
        ]
        + [pltpu.VMEM((NX, NX), bf16)] * 4
        + [
            pltpu.VMEM((chips, 2, py_count, 2 * ky_part + 8, width), s16),
            pltpu.VMEM((py_count, chips, 2, 2 * ky_part + 8, width), s16),
            pltpu.VMEM((2, 2 * rows, 2 * width), bf16),
            pltpu.VMEM((2, span, width), f32),
            dma((py_count, chips)),
            dma((py_count, chips)),
            dma((py_count, chips)),
            dma((py_count, chips)),
            dma((py_count,)),
            dma((py_count,)),
            dma((chips, 2, py_count)),
            dma((chips, 2, py_count)),
        ],
        compiler_params=pltpu.CompilerParams(
            collective_id=0, has_side_effects=True, vmem_limit_bytes=62 * 1024 * 1024
        ),
        name="exchange",
    )(grid, counts_row, *tables)


def local(cell_ids, offset_x, offset_y, mass, live, tile_owner, counts):
    px_count = lax.axis_size("px")
    py_count = lax.axis_size("py")
    row_count = NX // px_count
    col_count = NY // py_count
    parts = px_count // PLANES
    cells = cell_ids[0]
    owners = tile_owner[0]
    devices = px_count * py_count
    ky_part = NY // devices
    buckets = owners * PLANES + cells[:, 0] // (row_count * col_count)
    edges = jnp.arange(px_count * PLANES + 1, dtype=jnp.int32)
    starts = jnp.sum((buckets[None, :] < edges[:, None]).astype(jnp.int32), axis=1)

    grid = spread(
        starts, cells, owners, offset_x[0], offset_y[0], mass[0], live[0], row_count, col_count
    )
    bucket_count = counts.shape[-1]
    lane_tiles = NX // LANES
    if px_count == PLANES and lane_tiles % py_count == 0 and bucket_count <= LANES:
        width = lane_tiles // py_count * LANES
        counts_row = jnp.pad(counts.reshape(1, -1), ((2, 5), (0, width - bucket_count)))
        out, total, begin = exchange(grid, counts_row, dft_parts(), px_count, py_count)
        out = out.reshape(2, PLANES, ky_part, NX)
        spectrum = scaled(out, total[0, 0])
        return (spectrum, begin[:1, :bucket_count][None])
    grid = grid.transpose(0, 2, 1, 3).reshape(PLANES, col_count + 16, NX)
    height = col_count + 16
    width = NX // parts
    if parts > 1:
        grid = grid.reshape(PLANES, height, parts, width).transpose(0, 2, 1, 3)
    grid = grid.reshape(px_count // 2, 2, height, width)
    side = lax.axis_index("px") % 2
    keep = lax.dynamic_index_in_dim(grid, side, 1, keepdims=False)
    away = lax.dynamic_index_in_dim(grid, 1 - side, 1, keepdims=False)
    pairs = [(source, source ^ 1) for source in range(px_count)]
    summed = keep + lax.ppermute(away, "px", pairs)
    groups = [list(range(k, px_count, 2)) for k in range(2)]
    got = lax.all_to_all(
        coded_rows(summed, col_count + 8), "px", 0, 0, axis_index_groups=groups, tiled=True
    )
    mine = jnp.sum(plain_rows(got, col_count + 8), axis=0)
    total = jnp.sum(mine)
    by_cols = lax.all_to_all(
        coded_rows(mine, col_count + 8), "py", split_axis=1, concat_axis=0, tiled=True
    )
    part = width // py_count
    ext = plain_rows(by_cols.reshape(py_count, height, part), col_count + 8)
    core = ext[:, :col_count]
    right = jnp.roll(ext[:, col_count : col_count + 4], 1, axis=0)
    left = jnp.roll(ext[:, col_count + 12 :], -1, axis=0)
    core = core + jnp.concatenate(
        [right, jnp.zeros((py_count, col_count - 8, part), jnp.float32), left], axis=1
    )
    data = core.reshape(NY, part)
    cos_hi, cos_lo, sin_hi, sin_lo = dft_tables()
    hi, lo = split(data)
    both = jnp.concatenate([hi, lo], axis=1)
    real = dot(cos_hi, both)
    real = real[:, :part] + real[:, part:] + dot(cos_lo, hi)
    imag = dot(sin_hi, both)
    imag = -(imag[:, :part] + imag[:, part:] + dot(sin_lo, hi))
    lines = jnp.stack([real.reshape(devices, ky_part, part), imag.reshape(devices, ky_part, part)], 1)
    lines = lines.reshape(devices, 2 * ky_part, part)
    power = power_of(jnp.max(jnp.abs(lines), axis=1, keepdims=True))
    coded = coded_as(lines, power)
    count_rows = -(-bucket_count // part)
    spare = -(2 + count_rows) % 8
    side_rows = jnp.concatenate(
        [
            digits(total, part),
            jnp.pad(counts.reshape(-1), (0, count_rows * part - bucket_count)).reshape(-1, part),
            jnp.zeros((spare, part), jnp.int32),
        ]
    ).astype(jnp.int16)
    side_rows = jnp.broadcast_to(side_rows[None], (devices,) + side_rows.shape)
    coded = jnp.concatenate([coded, power.astype(jnp.int16), side_rows], axis=1)
    got = lax.all_to_all(coded, ("px", "py"), split_axis=0, concat_axis=0, tiled=True)
    after = got[:, 2 * ky_part :].astype(jnp.int32)
    lines = got[:, : 2 * ky_part].astype(jnp.float32) * scale_of(after[:, :1])
    total = jnp.sum(number(after[:, 1]))
    column = after[:, 2 : 2 + count_rows].reshape(px_count, py_count, 1, count_rows * part)
    column = lax.dynamic_index_in_dim(column, lax.axis_index("py"), 1, keepdims=False)
    column = column[:, :, :bucket_count][:, None]
    got = lines.reshape(PLANES, parts * py_count, 2, ky_part, part).transpose(2, 0, 3, 1, 4)
    got = got.reshape(2 * PLANES * ky_part, NX)
    hi, lo = split(got)
    rows = PLANES * ky_part
    both = jnp.concatenate([hi, lo], axis=0)
    by_cos = dot(both, cos_hi)
    by_cos = by_cos[: 2 * rows] + by_cos[2 * rows :] + dot(hi, cos_lo)
    by_sin = dot(both, sin_hi)
    by_sin = by_sin[: 2 * rows] + by_sin[2 * rows :] + dot(hi, sin_lo)
    out = jnp.stack([by_cos[:rows] + by_sin[rows:], by_cos[rows:] - by_sin[:rows]])
    out = out.reshape(2, PLANES, ky_part, NX)
    spectrum = scaled(out, total)
    column_sum = jnp.sum(column, axis=0)
    reached = lax.broadcasted_iota(jnp.int32, column.shape, 0) < lax.axis_index("px")
    earlier = jnp.sum(jnp.where(reached, column, 0), axis=0)
    preceding = jnp.cumsum(column_sum, axis=-1) - column_sum
    bucket_start = (preceding + earlier).astype(jnp.int32)
    return (spectrum, bucket_start)


def solution(mesh):
    placed = (
        P("px", "py", None),
        P("px", "py", None),
        P("px", "py", None),
        P("px", "py", None),
        P("px", "py", None),
        P("px", "py"),
        P("px", "py", None),
    )
    return jax.shard_map(
        local,
        mesh=mesh,
        in_specs=placed,
        out_specs=(P(None, None, ("px", "py"), None), P("px", "py", None)),
        check_vma=False,
    )
```

```python
import functools
import math

import jax
import jax.numpy as jnp
import numpy as np
from jax import lax
from jax.experimental import pallas as pl
from jax.experimental.pallas import tpu as pltpu
from jax.sharding import PartitionSpec as P

NX = 1024
NY = 1024
PLANES = 8
BETA = 18.4
LANES = 128
GROUP = 4
UNROLL = 8
EAGER = 3
SPREAD_VMEM = 24
EXCHANGE_VMEM = 34
RATE = BETA / math.log(2.0)


def tap_blocks(start, fraction, scaling, rows):
    depth = (rows - start + 3) & 7
    z = ((depth - 3).astype(jnp.float32) - fraction) * 0.25
    u = jnp.maximum(1.0 - z * z, 0.0)
    taps = jnp.exp2(u * lax.rsqrt(jnp.maximum(u, 1e-30)) * RATE - RATE)
    if scaling is not None:
        taps = taps * scaling
    at = start - 3 + depth
    odd = (at & 8) != 0
    zero = jnp.zeros_like(taps)
    both = jnp.concatenate(
        [jnp.where(odd, zero, taps), jnp.where(odd, taps, zero)], axis=0
    ).astype(jnp.bfloat16)
    return both, at >> 4


def placed_blocks(taps, block, count):
    block = jnp.where(block < 0, count, block)
    block = jnp.concatenate([block, block], axis=0).astype(jnp.int16)
    none = jnp.zeros_like(taps)
    return [jnp.where(block == k, taps, none) for k in range(count + 1)]


def spread_kernel(row_count, col_count, bucket_count, cell_in, owner_in, fx_in, fy_in, mass_in, live_in,
                  out_ref, rim_ref, owner_ref, x_ref, y_ref, w_ref, c_ref, fx_ref, fy_ref, mass_ref, live_ref,
                  edge_ref, starts_ref, item_ref, sems, edge_sem):
    tiles = cell_in.shape[0]
    col_blocks = col_count // 16
    lane_tiles = NX // LANES
    owners_tile = LANES // row_count if row_count < LANES else 1
    height = col_count + 16
    rows = lax.broadcasted_iota(jnp.int32, (8, LANES), 0)
    spare = pl.ds(tiles, 8)
    copies = [
        pltpu.make_async_copy(source, target, sems.at[k])
        for k, (source, target) in enumerate(
            (
                (cell_in, c_ref.at[pl.ds(0, tiles)]),
                (owner_in, owner_ref),
                (fx_in, fx_ref),
                (fy_in, fy_ref),
                (mass_in, mass_ref),
                (live_in, live_ref),
            )
        )
    ]
    for copy in copies:
        copy.start()
    for ref in (x_ref, y_ref, w_ref, c_ref):
        ref[spare, :] = jnp.zeros((8, LANES), ref.dtype)
    rim_ref[...] = jnp.zeros_like(rim_ref)

    copies[0].wait()
    copies[1].wait()
    plane_bits = (row_count * col_count).bit_length() - 1
    groups = edge_ref.shape[0]
    for g in range(groups):
        edge = lax.broadcasted_iota(jnp.int32, (LANES, LANES), 1) + g * LANES
        found = jnp.zeros((8, LANES), jnp.int32)
        for k in range(0, tiles, LANES):
            count = min(LANES, tiles - k)
            owner = jnp.broadcast_to(owner_ref[:, pl.ds(k, LANES)], (LANES, LANES)).T
            bucket = owner[:count] * PLANES + lax.shift_right_logical(
                c_ref[pl.ds(k, count), :], plane_bits
            )
            lower = jnp.where(bucket < edge[:count], 1, 0)
            for r in range(0, count, 8):
                found = found + lower[r : r + 8]
        edge_ref[pl.ds(g, 1), :] = jnp.sum(found, axis=0, keepdims=True)
    edges = pltpu.make_async_copy(edge_ref, starts_ref, edge_sem)
    edges.start()
    out_ref[...] = jnp.zeros_like(out_ref)
    for copy in copies[2:]:
        copy.wait()
    x_ref[pl.ds(0, tiles), :] = fx_ref[...].astype(jnp.float32)
    y_ref[pl.ds(0, tiles), :] = fy_ref[...].astype(jnp.float32)
    mass = mass_ref[...].astype(jnp.float32)
    w_ref[pl.ds(0, tiles), :] = jnp.where(live_ref[...] == 1, mass, jnp.zeros_like(mass))
    edges.wait()

    def start_of(b):
        return starts_ref[lax.shift_right_logical(b, 7), b & (LANES - 1)]

    def of_bucket(b, at):
        begin = start_of(b)
        count = (start_of(b + 1) - begin + GROUP - 1) // GROUP
        word = b * 65536 + begin
        for c in range(EAGER):
            item_ref[at + c] = word + c * GROUP

        @pl.when(count > EAGER)
        def _():
            def one(c, _):
                item_ref[at + c] = word + c * GROUP
                return 0

            lax.fori_loop(EAGER, count, one, 0)

        return at + count

    items = lax.fori_loop(0, bucket_count, of_bucket, 0)
    for k in range(UNROLL):
        item_ref[items + k] = (bucket_count - 1) * 65536 + tiles

    def product(k):
        begin = item_ref[k] & 65535
        bucket = lax.shift_right_logical(item_ref[k], 16)
        end = start_of(bucket + 1)
        shift = bucket // PLANES % owners_tile * row_count
        wxs, wys = [], []
        for g in range(GROUP):
            t = begin + g
            at = pl.ds(t, 1)
            scale = jnp.where(t < end, 1.0, 0.0)
            cell = jnp.broadcast_to(c_ref[at, :], (8, LANES))
            lx = lax.shift_right_logical(cell, col_count.bit_length() - 1) & (row_count - 1)
            if owners_tile > 1:
                lx = lx + shift
            taps, block = tap_blocks(lx, x_ref[at, :], None, rows)
            wxs.append(jnp.concatenate(placed_blocks(taps, block, LANES // 16), axis=0))
            taps, block = tap_blocks(cell & (col_count - 1), y_ref[at, :], w_ref[at, :] * scale, rows)
            wys.append(jnp.concatenate(placed_blocks(taps, block, col_blocks), axis=0))
        return lax.dot_general(
            jnp.concatenate(wys, axis=1), jnp.concatenate(wxs, axis=1),
            (((1,), (1,)), ((), ())), preferred_element_type=jnp.float32
        )

    def some(i, _):
        results = [product(i * UNROLL + u) for u in range(UNROLL)]
        for u, result in enumerate(results):
            b = lax.shift_right_logical(item_ref[i * UNROLL + u], 16)
            plane = b % PLANES
            tile = (b // PLANES * row_count) // LANES
            out_ref[plane, tile] += result[:, :LANES]
            rim_ref[plane, tile] += jnp.concatenate(
                [result[:, LANES:], jnp.zeros((height, LANES - 16), jnp.float32)], axis=1
            )
        return 0

    lax.fori_loop(0, (items + UNROLL - 1) // UNROLL, some, 0)

    lane = lax.broadcasted_iota(jnp.int32, (8, LANES), 1)

    def close(i, _):
        plane = i // 2
        for k in range(lane_tiles // 2):
            tile = i % 2 * (lane_tiles // 2) + k
            low = (tile + lane_tiles - 1) % lane_tiles
            high = (tile + 1) % lane_tiles
            for r in range(0, height, 8):
                at = pl.ds(r, 8)
                left = jnp.where(lane < 8, rim_ref[plane, low, at, :], 0.0)
                right = jnp.where(lane < 8, 0.0, rim_ref[plane, high, at, :])
                out_ref[plane, tile, at, :] += left + pltpu.roll(right, LANES - 16, 1)
        return 0

    lax.fori_loop(0, 2 * PLANES, close, 0)


def spread(cells, owners, fx, fy, mass, live, row_count, col_count, bucket_count):
    height = col_count + 16
    tiles = cells.shape[0]
    vmem = pl.BlockSpec(memory_space=pltpu.VMEM)
    anywhere = pl.BlockSpec(memory_space=pltpu.HBM)
    wide = -(-tiles // LANES) * LANES
    owners = jnp.pad(owners, ((0, 0), (0, wide - tiles)))
    edges = (-(-(bucket_count + 1) // LANES), LANES)
    return pl.pallas_call(
        functools.partial(spread_kernel, row_count, col_count, bucket_count),
        out_shape=jax.ShapeDtypeStruct((PLANES, NX // LANES, height, LANES), jnp.float32),
        in_specs=[anywhere] * 6,
        out_specs=vmem,
        scratch_shapes=[
            pltpu.VMEM((PLANES, NX // LANES, height, LANES), jnp.float32),
            pltpu.VMEM((1, wide), jnp.int32),
            pltpu.VMEM((tiles + 8, LANES), jnp.float32),
            pltpu.VMEM((tiles + 8, LANES), jnp.float32),
            pltpu.VMEM((tiles + 8, LANES), jnp.float32),
            pltpu.VMEM((tiles + 8, LANES), jnp.int32),
            pltpu.VMEM((tiles, LANES), fx.dtype),
            pltpu.VMEM((tiles, LANES), fy.dtype),
            pltpu.VMEM((tiles, LANES), mass.dtype),
            pltpu.VMEM((tiles, LANES), live.dtype),
            pltpu.VMEM(edges, jnp.int32),
            pltpu.SMEM(edges, jnp.int32),
            pltpu.SMEM((-(-tiles // GROUP) + bucket_count + UNROLL + EAGER,), jnp.int32),
            pltpu.SemaphoreType.DMA((6,)),
            pltpu.SemaphoreType.DMA,
        ],
        compiler_params=pltpu.CompilerParams(vmem_limit_bytes=SPREAD_VMEM * 1024 * 1024),
        name="spread",
    )(*(pltpu.with_memory_space_constraint(v, pltpu.HBM) for v in (cells, owners, fx, fy, mass, live)))


def split(value):
    high = lax.reduce_precision(value, 8, 7)
    return high.astype(jnp.bfloat16), (value - high).astype(jnp.bfloat16)


def dft_parts():
    n = np.arange(NX)
    k = np.arange(32)
    coarse = 2.0 * np.pi / NX * ((32 * k[:, None] * n[None, :]) % NX)
    fine = 2.0 * np.pi / NX * ((k[:, None] * n[None, :]) % NX)
    return tuple(jnp.asarray(f(a), jnp.float32) for a in (coarse, fine) for f in (np.cos, np.sin))


def dft_tables():
    cc, cs, fc, fs = lax.optimization_barrier(dft_parts())
    cc, cs = cc[:, None, :], cs[:, None, :]
    fc, fs = fc[None, :, :], fs[None, :, :]
    cosine = (cc * fc - cs * fs).reshape(NX, NX)
    sine = (cs * fc + cc * fs).reshape(NX, NX)
    return split(cosine) + split(sine)


def dot(a, b):
    return jnp.dot(a, b, preferred_element_type=jnp.float32)


def power_of(top):
    return jnp.clip(jnp.floor(jnp.log2(jnp.maximum(top, 1e-30))) + 1.0, -90.0, 90.0).astype(jnp.int32)


def scale_of(power):
    return jnp.exp2((power - 15).astype(jnp.float32))


def coded_as(value, power):
    steps = jnp.round(value * jnp.exp2((15 - power).astype(jnp.float32)))
    return jnp.clip(steps, -32767.0, 32767.0).astype(jnp.int16)


def coded_rows(value, spare):
    power = power_of(jnp.max(jnp.abs(value), axis=-2, keepdims=True))
    row = lax.broadcasted_iota(jnp.int32, value.shape, value.ndim - 2)
    return jnp.where(row == spare, power.astype(jnp.int16), coded_as(value, power))


def plain_rows(coded, spare):
    power = lax.slice_in_dim(coded, spare, spare + 1, axis=coded.ndim - 2).astype(jnp.int32)
    row = lax.broadcasted_iota(jnp.int32, coded.shape, coded.ndim - 2)
    return jnp.where(row == spare, 0.0, coded.astype(jnp.float32) * scale_of(power))


def digits(value, width):
    power = power_of(value)
    scaled = value * jnp.exp2((14 - power).astype(jnp.float32))
    high = jnp.clip(jnp.floor(scaled), 0.0, 32767.0)
    low = jnp.clip(jnp.floor((scaled - high) * 16384.0), 0.0, 16384.0)
    lane = lax.broadcasted_iota(jnp.int32, (1, width), 1)
    rest = jnp.where(lane == 1, high, low).astype(jnp.int32)
    return jnp.where(lane == 0, power, rest)


def number(row):
    value = row[..., 1].astype(jnp.float32) + row[..., 2].astype(jnp.float32) / 16384.0
    return value * jnp.exp2((row[..., 0] - 14).astype(jnp.float32))


def scaled(out, total):
    py_count = lax.axis_size("py")
    ky_part = out.shape[2]
    norm = 1.0 / math.sqrt(NX * NY)
    index = lax.axis_index("px") * py_count + lax.axis_index("py")
    shape = (2, 1, ky_part, NX)
    at_zero = (
        (lax.broadcasted_iota(jnp.int32, shape, 0) == 0)
        & (lax.broadcasted_iota(jnp.int32, shape, 2) + index == 0)
        & (lax.broadcasted_iota(jnp.int32, shape, 3) == 0)
    )
    return out * (PLANES * NX * NY * norm / total) - jnp.where(at_zero, NX * NY * norm, 0.0)


def code_power(top):
    return jnp.clip(jnp.floor(jnp.log2(jnp.maximum(top, 1e-30))) + 1.0, -90.0, 90.0)


def code_block(read, store, row_groups, spare):
    top = None
    for r in range(row_groups):
        here = jnp.abs(read(r))
        top = here if top is None else jnp.maximum(top, here)
    power = code_power(jnp.max(top, axis=0, keepdims=True))
    factor = jnp.exp2(15.0 - power)
    for r in range(row_groups):
        steps = jnp.clip(jnp.round(read(r) * factor), -32767.0, 32767.0)
        if r == row_groups - 1 and spare is not None:
            row = lax.broadcasted_iota(jnp.int32, steps.shape, 0)
            steps = jnp.where(row == spare, power, steps)
        store(r, steps.astype(jnp.int32).astype(jnp.int16))
    return power


def exchange_kernel(px_count, py_count, grid_ref, counts_ref, coarse_c_in, coarse_s_in, fine_c_in,
                    fine_s_in, out_ref, starts_ref,
                    coarse_c_ref, coarse_s_ref, fine_c_ref, fine_s_ref, side_ref, table_sems,
                    pair_ref, own_ref, code_ref, got_ref, zcode_ref, zgot_ref, data_ref, dhl_ref,
                    chi_ref, clo_ref, shi_ref, slo_ref, fcode_ref, fgot_ref, lhs_ref, line_ref,
                    pair_send, pair_recv, code_send, code_recv, z_send, z_recv, f_send, f_recv):
    px = lax.axis_index("px")
    py = lax.axis_index("py")
    core = px % 2
    chip = px // 2
    chips = px_count // 2
    other = px + 1 - 2 * core
    blocks, tiles, height, _ = grid_ref.shape
    part = tiles // py_count
    col_count = height - 16
    groups = height // 16
    spare = 8
    width = part * LANES
    devices = px_count * py_count
    ky_part = NY // devices

    tables = [
        pltpu.make_async_copy(source, target, table_sems.at[k])
        for k, (source, target) in enumerate(
            (
                (coarse_c_in, coarse_c_ref),
                (coarse_s_in, coarse_s_ref),
                (fine_c_in, fine_c_ref),
                (fine_s_in, fine_s_ref),
            )
        )
    ]
    for copy in tables:
        copy.start()
    barrier = pltpu.get_barrier_semaphore()
    for e in range(2):
        for s in range(chips):
            for m in range(py_count):
                if e + s + m > 0:
                    to = ((chip + s) % chips * 2 + (core + e) % 2, (py + m) % py_count)
                    pl.semaphore_signal(barrier, inc=1, device_id=to, device_id_type=pl.DeviceIdType.MESH)
    pl.semaphore_wait(barrier, devices - 1)

    order = [(m, s) for m in range(py_count - 1, -1, -1) for s in range(chips - 1, -1, -1)]

    def pair_copy(m, s):
        q = (py + m) % py_count
        block = (chip + s) % chips * 2
        return pltpu.make_async_remote_copy(
            src_ref=grid_ref.at[block + 1 - core, pl.ds(q * part, part)],
            dst_ref=pair_ref.at[m, s],
            send_sem=pair_send.at[m, s],
            recv_sem=pair_recv.at[m, s],
            device_id=(other, py),
            device_id_type=pl.DeviceIdType.MESH,
        )

    def code_copy(m, s):
        return pltpu.make_async_remote_copy(
            src_ref=code_ref.at[m, s],
            dst_ref=got_ref.at[m, s],
            send_sem=code_send.at[m, s],
            recv_sem=code_recv.at[m, s],
            device_id=((chip + s) % chips * 2 + core, py),
            device_id_type=pl.DeviceIdType.MESH,
        )

    def z_copy(m):
        return pltpu.make_async_remote_copy(
            src_ref=zcode_ref.at[m],
            dst_ref=zgot_ref.at[m],
            send_sem=z_send.at[m],
            recv_sem=z_recv.at[m],
            device_id=(px, (py + m) % py_count),
            device_id_type=pl.DeviceIdType.MESH,
        )

    def f_copy(s, e, m):
        return pltpu.make_async_remote_copy(
            src_ref=fcode_ref.at[s, e, m],
            dst_ref=fgot_ref.at[m, s, e],
            send_sem=f_send.at[s, e, m],
            recv_sem=f_recv.at[s, e, m],
            device_id=((chip + s) % chips * 2 + (core + e) % 2, (py + m) % py_count),
            device_id_type=pl.DeviceIdType.MESH,
        )

    for m, s in order:
        pair_copy(m, s).start()

    for m, s in order:
        pair_copy(m, s).wait_recv()
        q = (py + m) % py_count
        block = (chip + s) % chips * 2 + core

        def add(t, _):
            def summed(r):
                at = pl.ds(r * 16, 16)
                return grid_ref[block, q * part + t, at, :] + pair_ref[m, s, t, at, :]

            if s == 0:
                for r in range(groups):
                    own_ref[m, t, pl.ds(r * 16, 16), :] = summed(r)
            else:
                def keep(r, value):
                    code_ref[m, s, t, pl.ds(r * 16, 16), :] = value

                code_block(summed, keep, groups, spare)
            return 0

        lax.fori_loop(0, part, add, 0)
        if s > 0:
            code_copy(m, s).start()

    for copy in tables:
        copy.wait()
    def table(a, _):
        at = pl.ds(pl.multiple_of(a * 32, 32), 32)
        cc = coarse_c_ref[pl.ds(a, 1), :]
        cs = coarse_s_ref[pl.ds(a, 1), :]
        fc = fine_c_ref[...]
        fs = fine_s_ref[...]
        for value, high_ref, low_ref in (
            (cc * fc - cs * fs, chi_ref, clo_ref),
            (cs * fc + cc * fs, shi_ref, slo_ref),
        ):
            high = value.astype(jnp.bfloat16)
            high_ref[at, :] = high
            low_ref[at, :] = (value - high.astype(jnp.float32)).astype(jnp.bfloat16)
        return 0

    lax.fori_loop(0, NX // 32, table, 0)

    def scale_from(rows):
        return jnp.exp2(rows[8:9].astype(jnp.float32) - 15.0)

    def plain(ref_at, r):
        return ref_at(r).astype(jnp.int32).astype(jnp.float32)

    row16 = lax.broadcasted_iota(jnp.int32, (16, LANES), 0)
    total = jnp.zeros((16, LANES), jnp.float32)
    for m in range(py_count - 1, -1, -1):
        for s in range(chips - 1, 0, -1):
            code_copy(m, s).wait_recv()

        def gather(t, total):
            scales = [
                jnp.exp2(got_ref[m, s, t, pl.ds(col_count, 16), :].astype(jnp.int32)[8:9].astype(jnp.float32) - 15.0)
                for s in range(1, chips)
            ]

            for r in range(groups):
                at = pl.ds(r * 16, 16)
                value = own_ref[m, t, at, :]
                for s in range(1, chips):
                    term = got_ref[m, s, t, at, :].astype(jnp.int32).astype(jnp.float32) * scales[s - 1]
                    if r == groups - 1:
                        term = jnp.where(row16 == spare, 0.0, term)
                    value = value + term
                own_ref[m, t, at, :] = value
                total = total + value
            if m > 0:
                def keep(r, value):
                    zcode_ref[m, t, pl.ds(r * 16, 16), :] = value

                code_block(lambda r: own_ref[m, t, pl.ds(r * 16, 16), :], keep, groups, spare)
            return total

        total = lax.fori_loop(0, part, gather, total)
        if m > 0:
            z_copy(m).start()

    total = jnp.sum(total)

    def place(m, reader):
        source = (py + py_count - m) % py_count
        for t in range(part):
            cols = pl.ds(t * LANES, LANES)
            for r in range(groups - 1):
                data_ref[source, pl.ds(r * 16, 16), cols] = reader(t, r)

    def rims(m, reader):
        source = (py + py_count - m) % py_count
        after = (source + 1) % py_count
        before = (source + py_count - 1) % py_count
        for t in range(part):
            cols = pl.ds(t * LANES, LANES)
            rim = reader(t, groups - 1)
            low = pl.ds(0, 8)
            high = pl.ds(col_count - 8, 8)
            row = lax.broadcasted_iota(jnp.int32, (8, LANES), 0)
            data_ref[after, low, cols] += jnp.where(row < 4, rim[:8], 0.0)
            data_ref[before, high, cols] += jnp.where(row > 4, rim[8:], 0.0)

    def own_reader(t, r):
        return own_ref[0, t, pl.ds(r * 16, 16), :]

    def z_reader(m):
        def read(t, r):
            scale = jnp.exp2(zgot_ref[m, t, pl.ds(col_count, 16), :].astype(jnp.int32)[8:9].astype(jnp.float32) - 15.0)
            return zgot_ref[m, t, pl.ds(r * 16, 16), :].astype(jnp.int32).astype(jnp.float32) * scale
        return read

    readers = [own_reader] + [z_reader(m) for m in range(1, py_count)]
    place(0, readers[0])
    for m in range(py_count - 1, 0, -1):
        z_copy(m).wait_recv()
        place(m, readers[m])
    for m in range(py_count):
        rims(m, readers[m])
    for j in range(py_count):
        def halves(r, _):
            at = pl.ds(pl.multiple_of(r * 16, 16), 16)
            value = data_ref[j, at, :]
            high = value.astype(jnp.bfloat16)
            to = pl.ds(pl.multiple_of(j * col_count + r * 16, 16), 16)
            dhl_ref[0, to, :] = high
            dhl_ref[1, to, :] = (value - high.astype(jnp.float32)).astype(jnp.bfloat16)
            return 0

        lax.fori_loop(0, col_count // 16, halves, 0)

    power = code_power(total)
    scaled = total * jnp.exp2(14.0 - power)
    first = jnp.clip(jnp.floor(scaled), 0.0, 32767.0)
    second = jnp.clip(jnp.floor((scaled - first) * 16384.0), 0.0, 16384.0)
    row8 = lax.broadcasted_iota(jnp.int32, (8, width), 0)
    lane8 = lax.broadcasted_iota(jnp.int32, (8, width), 1)
    number = jnp.where(lane8 == 0, power, jnp.where(lane8 == 1, first, second))
    bucket_count = counts_ref.shape[1]
    side_ref[...] = jnp.where(row8 == 1, number, 0.0)
    side_ref[pl.ds(2, 1), pl.ds(0, bucket_count)] = counts_ref[...].astype(jnp.float32)
    side = side_ref[...]
    span = 2 * py_count * ky_part

    def transform(s):
        at = pl.ds(pl.multiple_of((chip + s) % chips * span, span), span)
        for high_ref, low_ref, k in ((chi_ref, clo_ref, 0), (shi_ref, slo_ref, 1)):
            value = jnp.dot(high_ref[at, :], dhl_ref[0], preferred_element_type=jnp.float32)
            value += jnp.dot(high_ref[at, :], dhl_ref[1], preferred_element_type=jnp.float32)
            value += jnp.dot(low_ref[at, :], dhl_ref[0], preferred_element_type=jnp.float32)
            line_ref[k] = value if k == 0 else -value
        for e in range(2):
            for m in range(py_count):
                index = (core + e) % 2 * py_count + (py + m) % py_count
                rows = pl.ds(pl.multiple_of(index * ky_part, ky_part), ky_part)
                real = line_ref[0, rows, :]
                imag = line_ref[1, rows, :]
                top = jnp.maximum(jnp.abs(real), jnp.abs(imag))
                power = code_power(jnp.max(top, axis=0, keepdims=True))
                factor = jnp.exp2(15.0 - power)
                for k, value in enumerate((real, imag)):
                    steps = jnp.clip(jnp.round(value * factor), -32767.0, 32767.0)
                    fcode_ref[s, e, m, pl.ds(k * ky_part, ky_part), :] = steps.astype(jnp.int32).astype(jnp.int16)
                rest = jnp.where(row8 == 0, power, side)
                fcode_ref[s, e, m, pl.ds(2 * ky_part, 8), :] = rest.astype(jnp.int32).astype(jnp.int16)

    def send_all(s):
        transform(s)
        for e in range(2):
            for m in range(py_count - 1, -1, -1):
                f_copy(s, e, m).start()
        return 0

    lax.fori_loop(0, chips - 1, lambda k, _: send_all(chips - 1 - k), 0)
    transform(0)
    for e in range(1, -1, -1):
        for m in range(py_count - 1, -1, -1):
            if e + m > 0:
                f_copy(0, e, m).start()

    sum_total = total
    column = jnp.zeros((8, width), jnp.float32)
    before = jnp.zeros((8, width), jnp.float32)
    rows_all = px_count * ky_part
    for m in range(py_count):
        source = (py + py_count - m) % py_count
        for s in range(chips):
            for e in range(2):
                mine = m + s + e == 0
                if not mine:
                    f_copy(s, e, m).wait_recv()
                got = fcode_ref if mine else fgot_ref
                where = (0, 0, 0) if mine else (m, s, e)
                sender = (chip + chips - s) % chips * 2 + (core + e) % 2
                rest = got[where + (pl.ds(2 * ky_part, 8), slice(None))].astype(jnp.int32)
                scale = jnp.exp2(rest[0:1].astype(jnp.float32) - 15.0)
                info = rest.astype(jnp.float32)
                if not mine:
                    digit = info[1:2, :LANES]
                    lane1 = lax.broadcasted_iota(jnp.int32, (1, LANES), 1)
                    body = jnp.sum(jnp.where(lane1 == 1, digit, 0.0) + jnp.where(lane1 == 2, digit * (1.0 / 16384.0), 0.0))
                    bits = jnp.sum(jnp.where(lane1 == 0, digit, 0.0))
                    sum_total = sum_total + body * jnp.exp2(bits - 14.0)
                if m == 0:
                    column = column + info
                    before = before + jnp.where(sender < px, info, 0.0)
                rows = pl.ds(pl.multiple_of(sender * ky_part, ky_part), ky_part)
                rows2 = pl.ds(pl.multiple_of(rows_all + sender * ky_part, ky_part), ky_part)
                real = got[where + (pl.ds(0, ky_part), slice(None))].astype(jnp.int32).astype(jnp.float32) * scale
                imag = got[where + (pl.ds(ky_part, ky_part), slice(None))].astype(jnp.int32).astype(jnp.float32) * scale
                for at, a, b in ((rows, real, imag), (rows2, imag, -real)):
                    for k, value in enumerate((a, b)):
                        high = value.astype(jnp.bfloat16)
                        lhs_ref[0, at, pl.ds(k * width, width)] = high
                        lhs_ref[1, at, pl.ds(k * width, width)] = (value - high.astype(jnp.float32)).astype(jnp.bfloat16)

        norm = 1.0 / math.sqrt(NX * NY)
        factor = (PLANES * NX * NY * norm) / jnp.full((1, 256), sum_total, jnp.float32)
        xrows = pl.ds(pl.multiple_of(source * width, width), width)

        def columns(n, _):
            cols = pl.ds(pl.multiple_of(n * 256, 256), 256)
            high = lhs_ref[0]
            low = lhs_ref[1]
            ch, cl, sh, sl = (ref[xrows, cols] for ref in (chi_ref, clo_ref, shi_ref, slo_ref))
            hh = jnp.concatenate([ch, sh], axis=0)
            ll = jnp.concatenate([cl, sl], axis=0)
            value = jnp.dot(high, hh, preferred_element_type=jnp.float32)
            value += jnp.dot(low, hh, preferred_element_type=jnp.float32)
            value += jnp.dot(high, ll, preferred_element_type=jnp.float32)
            if m > 0:
                value += out_ref[:, cols]
            if m == py_count - 1:
                value = value * factor
            out_ref[:, cols] = value
            return 0

        lax.fori_loop(0, NX // 256, columns, 0)

    first8 = lax.broadcasted_iota(jnp.int32, (8, LANES), 0) == 0
    corner = first8 & (lax.broadcasted_iota(jnp.int32, (8, LANES), 1) + px + py == 0)
    for plane in range(px_count):
        at = pl.ds(plane * ky_part, 8)
        out_ref[at, pl.ds(0, LANES)] -= jnp.where(corner, NX * NY * norm, 0.0)
    sums = column[2:3]
    lane = lax.broadcasted_iota(jnp.int32, (1, width), 1)
    preceding = sums
    step = 1
    while step < width:
        preceding = preceding + jnp.where(lane >= step, pltpu.roll(preceding, step, 1), 0.0)
        step *= 2
    begin = (preceding - sums + before[2:3]).astype(jnp.int32)
    starts_ref[0] = begin[:, :bucket_count]

    for m, s in order:
        pair_copy(m, s).wait_send()
        if s > 0:
            code_copy(m, s).wait_send()
    for m in range(1, py_count):
        z_copy(m).wait_send()
    for s in range(chips):
        for e in range(2):
            for m in range(py_count):
                if s + e + m > 0:
                    f_copy(s, e, m).wait_send()


def exchange(grid, counts, tables, px_count, py_count):
    blocks, tiles, height, _ = grid.shape
    chips = px_count // 2
    part = tiles // py_count
    width = part * LANES
    col_count = height - 16
    ky_part = NY // (px_count * py_count)
    span = 2 * py_count * ky_part
    rows = px_count * ky_part
    vmem = pl.BlockSpec(memory_space=pltpu.VMEM)
    dma = pltpu.SemaphoreType.DMA
    f32, bf16, s16 = jnp.float32, jnp.bfloat16, jnp.int16
    return pl.pallas_call(
        functools.partial(exchange_kernel, px_count, py_count),
        out_shape=(
            jax.ShapeDtypeStruct((2 * rows, NX), f32),
            jax.ShapeDtypeStruct((1,) + counts.shape, jnp.int32),
        ),
        in_specs=[vmem] * 2 + [pl.BlockSpec(memory_space=pltpu.HBM)] * 4,
        out_specs=[vmem] * 2,
        scratch_shapes=[pltpu.VMEM((32, NX), f32)] * 4
        + [
            pltpu.VMEM((8, width), f32),
            dma((4,)),
            pltpu.VMEM((py_count, chips, part, height, LANES), f32),
            pltpu.VMEM((py_count, part, height, LANES), f32),
            pltpu.VMEM((py_count, chips, part, height, LANES), s16),
            pltpu.VMEM((py_count, chips, part, height, LANES), s16),
            pltpu.VMEM((py_count, part, height, LANES), s16),
            pltpu.VMEM((py_count, part, height, LANES), s16),
            pltpu.VMEM((py_count, col_count, width), f32),
            pltpu.VMEM((2, NY, width), bf16),
        ]
        + [pltpu.VMEM((NX, NX), bf16)] * 4
        + [
            pltpu.VMEM((chips, 2, py_count, 2 * ky_part + 8, width), s16),
            pltpu.VMEM((py_count, chips, 2, 2 * ky_part + 8, width), s16),
            pltpu.VMEM((2, 2 * rows, 2 * width), bf16),
            pltpu.VMEM((2, span, width), f32),
            dma((py_count, chips)),
            dma((py_count, chips)),
            dma((py_count, chips)),
            dma((py_count, chips)),
            dma((py_count,)),
            dma((py_count,)),
            dma((chips, 2, py_count)),
            dma((chips, 2, py_count)),
        ],
        compiler_params=pltpu.CompilerParams(
            collective_id=0, has_side_effects=True, vmem_limit_bytes=EXCHANGE_VMEM * 1024 * 1024
        ),
        name="exchange",
    )(grid, counts, *tables)


def local(cell_ids, offset_x, offset_y, mass, live, tile_owner, counts):
    px_count = lax.axis_size("px")
    py_count = lax.axis_size("py")
    row_count = NX // px_count
    col_count = NY // py_count
    parts = px_count // PLANES
    devices = px_count * py_count
    ky_part = NY // devices
    grid = spread(
        cell_ids[0], tile_owner, offset_x[0], offset_y[0], mass[0], live[0], row_count, col_count,
        px_count * PLANES,
    )
    bucket_count = counts.shape[-1]
    lane_tiles = NX // LANES
    if px_count == PLANES and lane_tiles % py_count == 0 and bucket_count <= LANES:
        out, begin = exchange(grid, counts[0], dft_parts(), px_count, py_count)
        return (out.reshape(2, PLANES, ky_part, NX), begin)
    grid = grid.transpose(0, 2, 1, 3).reshape(PLANES, col_count + 16, NX)
    height = col_count + 16
    width = NX // parts
    if parts > 1:
        grid = grid.reshape(PLANES, height, parts, width).transpose(0, 2, 1, 3)
    grid = grid.reshape(px_count // 2, 2, height, width)
    side = lax.axis_index("px") % 2
    keep = lax.dynamic_index_in_dim(grid, side, 1, keepdims=False)
    away = lax.dynamic_index_in_dim(grid, 1 - side, 1, keepdims=False)
    pairs = [(source, source ^ 1) for source in range(px_count)]
    summed = keep + lax.ppermute(away, "px", pairs)
    groups = [list(range(k, px_count, 2)) for k in range(2)]
    got = lax.all_to_all(
        coded_rows(summed, col_count + 8), "px", 0, 0, axis_index_groups=groups, tiled=True
    )
    mine = jnp.sum(plain_rows(got, col_count + 8), axis=0)
    total = jnp.sum(mine)
    by_cols = lax.all_to_all(
        coded_rows(mine, col_count + 8), "py", split_axis=1, concat_axis=0, tiled=True
    )
    part = width // py_count
    ext = plain_rows(by_cols.reshape(py_count, height, part), col_count + 8)
    core = ext[:, :col_count]
    right = jnp.roll(ext[:, col_count : col_count + 4], 1, axis=0)
    left = jnp.roll(ext[:, col_count + 12 :], -1, axis=0)
    core = core + jnp.concatenate(
        [right, jnp.zeros((py_count, col_count - 8, part), jnp.float32), left], axis=1
    )
    data = core.reshape(NY, part)
    cos_hi, cos_lo, sin_hi, sin_lo = dft_tables()
    hi, lo = split(data)
    both = jnp.concatenate([hi, lo], axis=1)
    real = dot(cos_hi, both)
    real = real[:, :part] + real[:, part:] + dot(cos_lo, hi)
    imag = dot(sin_hi, both)
    imag = -(imag[:, :part] + imag[:, part:] + dot(sin_lo, hi))
    lines = jnp.stack([real.reshape(devices, ky_part, part), imag.reshape(devices, ky_part, part)], 1)
    lines = lines.reshape(devices, 2 * ky_part, part)
    power = power_of(jnp.max(jnp.abs(lines), axis=1, keepdims=True))
    coded = coded_as(lines, power)
    count_rows = -(-bucket_count // part)
    spare = -(2 + count_rows) % 8
    side_rows = jnp.concatenate(
        [
            digits(total, part),
            jnp.pad(counts.reshape(-1), (0, count_rows * part - bucket_count)).reshape(-1, part),
            jnp.zeros((spare, part), jnp.int32),
        ]
    ).astype(jnp.int16)
    side_rows = jnp.broadcast_to(side_rows[None], (devices,) + side_rows.shape)
    coded = jnp.concatenate([coded, power.astype(jnp.int16), side_rows], axis=1)
    got = lax.all_to_all(coded, ("px", "py"), split_axis=0, concat_axis=0, tiled=True)
    after = got[:, 2 * ky_part :].astype(jnp.int32)
    lines = got[:, : 2 * ky_part].astype(jnp.float32) * scale_of(after[:, :1])
    total = jnp.sum(number(after[:, 1]))
    column = after[:, 2 : 2 + count_rows].reshape(px_count, py_count, 1, count_rows * part)
    column = lax.dynamic_index_in_dim(column, lax.axis_index("py"), 1, keepdims=False)
    column = column[:, :, :bucket_count][:, None]
    got = lines.reshape(PLANES, parts * py_count, 2, ky_part, part).transpose(2, 0, 3, 1, 4)
    got = got.reshape(2 * PLANES * ky_part, NX)
    hi, lo = split(got)
    rows = PLANES * ky_part
    both = jnp.concatenate([hi, lo], axis=0)
    by_cos = dot(both, cos_hi)
    by_cos = by_cos[: 2 * rows] + by_cos[2 * rows :] + dot(hi, cos_lo)
    by_sin = dot(both, sin_hi)
    by_sin = by_sin[: 2 * rows] + by_sin[2 * rows :] + dot(hi, sin_lo)
    out = jnp.stack([by_cos[:rows] + by_sin[rows:], by_cos[rows:] - by_sin[:rows]])
    out = out.reshape(2, PLANES, ky_part, NX)
    spectrum = scaled(out, total)
    column_sum = jnp.sum(column, axis=0)
    reached = lax.broadcasted_iota(jnp.int32, column.shape, 0) < lax.axis_index("px")
    earlier = jnp.sum(jnp.where(reached, column, 0), axis=0)
    preceding = jnp.cumsum(column_sum, axis=-1) - column_sum
    bucket_start = (preceding + earlier).astype(jnp.int32)
    return (spectrum, bucket_start)


def solution(mesh):
    placed = (
        P("px", "py", None),
        P("px", "py", None),
        P("px", "py", None),
        P("px", "py", None),
        P("px", "py", None),
        P("px", "py"),
        P("px", "py", None),
    )
    return jax.shard_map(
        local,
        mesh=mesh,
        in_specs=placed,
        out_specs=(P(None, None, ("px", "py"), None), P("px", "py", None)),
        check_vma=False,
    )
```

```python
import functools
import math

import jax
import jax.numpy as jnp
import numpy as np
from jax import lax
from jax.experimental import pallas as pl
from jax.experimental.pallas import tpu as pltpu
from jax.sharding import PartitionSpec as P

NX = 1024
NY = 1024
PLANES = 8
BETA = 18.4
LANES = 128
GROUP = 4
UNROLL = 8
EAGER = 3
SPREAD_VMEM = 24
EXCHANGE_VMEM = 38
WIDE = 256
SENDS = (3, 2, 1, 0)
TAKES = (3, 0, 1, 2)
RATE = BETA / math.log(2.0)


def tap_blocks(start, fraction, scaling, rows):
    depth = (rows - start + 3) & 7
    z = ((depth - 3).astype(jnp.float32) - fraction) * 0.25
    u = jnp.maximum(1.0 - z * z, 0.0)
    taps = jnp.exp2(u * lax.rsqrt(jnp.maximum(u, 1e-30)) * RATE - RATE)
    if scaling is not None:
        taps = taps * scaling
    at = start - 3 + depth
    odd = (at & 8) != 0
    zero = jnp.zeros_like(taps)
    both = jnp.concatenate(
        [jnp.where(odd, zero, taps), jnp.where(odd, taps, zero)], axis=0
    ).astype(jnp.bfloat16)
    return both, at >> 4


def placed_blocks(taps, block, count):
    block = jnp.where(block < 0, count, block)
    block = jnp.concatenate([block, block], axis=0).astype(jnp.int16)
    none = jnp.zeros_like(taps)
    return [jnp.where(block == k, taps, none) for k in range(count + 1)]


def spread_kernel(row_count, col_count, bucket_count, cell_in, owner_in, fx_in, fy_in, mass_in, live_in,
                  out_ref, rim_ref, owner_ref, x_ref, y_ref, w_ref, c_ref, fx_ref, fy_ref, mass_ref, live_ref,
                  edge_ref, starts_ref, item_ref, sems, edge_sem):
    tiles = cell_in.shape[0]
    col_blocks = col_count // 16
    lane_tiles = NX // LANES
    owners_tile = LANES // row_count if row_count < LANES else 1
    height = col_count + 16
    rows = lax.broadcasted_iota(jnp.int32, (8, LANES), 0)
    spare = pl.ds(tiles, 8)
    copies = [
        pltpu.make_async_copy(source, target, sems.at[k])
        for k, (source, target) in enumerate(
            (
                (cell_in, c_ref.at[pl.ds(0, tiles)]),
                (owner_in, owner_ref),
                (fx_in, fx_ref),
                (fy_in, fy_ref),
                (mass_in, mass_ref),
                (live_in, live_ref),
            )
        )
    ]
    for copy in copies:
        copy.start()
    for ref in (x_ref, y_ref, w_ref, c_ref):
        ref[spare, :] = jnp.zeros((8, LANES), ref.dtype)
    rim_ref[...] = jnp.zeros_like(rim_ref)

    copies[0].wait()
    copies[1].wait()
    plane_bits = (row_count * col_count).bit_length() - 1
    groups = edge_ref.shape[0]
    for g in range(groups):
        edge = lax.broadcasted_iota(jnp.int32, (LANES, LANES), 1) + g * LANES
        found = jnp.zeros((8, LANES), jnp.int32)
        for k in range(0, tiles, LANES):
            count = min(LANES, tiles - k)
            owner = jnp.broadcast_to(owner_ref[:, pl.ds(k, LANES)], (LANES, LANES)).T
            bucket = owner[:count] * PLANES + lax.shift_right_logical(
                c_ref[pl.ds(k, count), :], plane_bits
            )
            lower = jnp.where(bucket < edge[:count], 1, 0)
            for r in range(0, count, 8):
                found = found + lower[r : r + 8]
        edge_ref[pl.ds(g, 1), :] = jnp.sum(found, axis=0, keepdims=True)
    edges = pltpu.make_async_copy(edge_ref, starts_ref, edge_sem)
    edges.start()
    out_ref[...] = jnp.zeros_like(out_ref)
    for copy in copies[2:]:
        copy.wait()
    x_ref[pl.ds(0, tiles), :] = fx_ref[...].astype(jnp.float32)
    y_ref[pl.ds(0, tiles), :] = fy_ref[...].astype(jnp.float32)
    mass = mass_ref[...].astype(jnp.float32)
    w_ref[pl.ds(0, tiles), :] = jnp.where(live_ref[...] == 1, mass, jnp.zeros_like(mass))
    edges.wait()

    def start_of(b):
        return starts_ref[lax.shift_right_logical(b, 7), b & (LANES - 1)]

    def of_bucket(b, at):
        begin = start_of(b)
        count = (start_of(b + 1) - begin + GROUP - 1) // GROUP
        word = b * 65536 + begin
        for c in range(EAGER):
            item_ref[at + c] = word + c * GROUP

        @pl.when(count > EAGER)
        def _():
            def one(c, _):
                item_ref[at + c] = word + c * GROUP
                return 0

            lax.fori_loop(EAGER, count, one, 0)

        return at + count

    items = lax.fori_loop(0, bucket_count, of_bucket, 0)
    for k in range(UNROLL):
        item_ref[items + k] = (bucket_count - 1) * 65536 + tiles

    def product(k):
        begin = item_ref[k] & 65535
        bucket = lax.shift_right_logical(item_ref[k], 16)
        end = start_of(bucket + 1)
        shift = bucket // PLANES % owners_tile * row_count
        wxs, wys = [], []
        for g in range(GROUP):
            t = begin + g
            at = pl.ds(t, 1)
            scale = jnp.where(t < end, 1.0, 0.0)
            cell = jnp.broadcast_to(c_ref[at, :], (8, LANES))
            lx = lax.shift_right_logical(cell, col_count.bit_length() - 1) & (row_count - 1)
            if owners_tile > 1:
                lx = lx + shift
            taps, block = tap_blocks(lx, x_ref[at, :], None, rows)
            wxs.append(jnp.concatenate(placed_blocks(taps, block, LANES // 16), axis=0))
            taps, block = tap_blocks(cell & (col_count - 1), y_ref[at, :], w_ref[at, :] * scale, rows)
            wys.append(jnp.concatenate(placed_blocks(taps, block, col_blocks), axis=0))
        return lax.dot_general(
            jnp.concatenate(wys, axis=1), jnp.concatenate(wxs, axis=1),
            (((1,), (1,)), ((), ())), preferred_element_type=jnp.float32
        )

    def some(i, _):
        results = [product(i * UNROLL + u) for u in range(UNROLL)]
        for u, result in enumerate(results):
            b = lax.shift_right_logical(item_ref[i * UNROLL + u], 16)
            plane = b % PLANES
            tile = (b // PLANES * row_count) // LANES
            out_ref[plane, tile] += result[:, :LANES]
            rim_ref[plane, tile] += jnp.concatenate(
                [result[:, LANES:], jnp.zeros((height, LANES - 16), jnp.float32)], axis=1
            )
        return 0

    lax.fori_loop(0, (items + UNROLL - 1) // UNROLL, some, 0)

    lane = lax.broadcasted_iota(jnp.int32, (8, LANES), 1)

    def close(i, _):
        plane = i // 2
        for k in range(lane_tiles // 2):
            tile = i % 2 * (lane_tiles // 2) + k
            low = (tile + lane_tiles - 1) % lane_tiles
            high = (tile + 1) % lane_tiles
            for r in range(0, height, 8):
                at = pl.ds(r, 8)
                left = jnp.where(lane < 8, rim_ref[plane, low, at, :], 0.0)
                right = jnp.where(lane < 8, 0.0, rim_ref[plane, high, at, :])
                out_ref[plane, tile, at, :] += left + pltpu.roll(right, LANES - 16, 1)
        return 0

    lax.fori_loop(0, 2 * PLANES, close, 0)


def spread(cells, owners, fx, fy, mass, live, row_count, col_count, bucket_count):
    height = col_count + 16
    tiles = cells.shape[0]
    vmem = pl.BlockSpec(memory_space=pltpu.VMEM)
    anywhere = pl.BlockSpec(memory_space=pltpu.HBM)
    wide = -(-tiles // LANES) * LANES
    owners = jnp.pad(owners, ((0, 0), (0, wide - tiles)))
    edges = (-(-(bucket_count + 1) // LANES), LANES)
    return pl.pallas_call(
        functools.partial(spread_kernel, row_count, col_count, bucket_count),
        out_shape=jax.ShapeDtypeStruct((PLANES, NX // LANES, height, LANES), jnp.float32),
        in_specs=[anywhere] * 6,
        out_specs=vmem,
        scratch_shapes=[
            pltpu.VMEM((PLANES, NX // LANES, height, LANES), jnp.float32),
            pltpu.VMEM((1, wide), jnp.int32),
            pltpu.VMEM((tiles + 8, LANES), jnp.float32),
            pltpu.VMEM((tiles + 8, LANES), jnp.float32),
            pltpu.VMEM((tiles + 8, LANES), jnp.float32),
            pltpu.VMEM((tiles + 8, LANES), jnp.int32),
            pltpu.VMEM((tiles, LANES), fx.dtype),
            pltpu.VMEM((tiles, LANES), fy.dtype),
            pltpu.VMEM((tiles, LANES), mass.dtype),
            pltpu.VMEM((tiles, LANES), live.dtype),
            pltpu.VMEM(edges, jnp.int32),
            pltpu.SMEM(edges, jnp.int32),
            pltpu.SMEM((-(-tiles // GROUP) + bucket_count + UNROLL + EAGER,), jnp.int32),
            pltpu.SemaphoreType.DMA((6,)),
            pltpu.SemaphoreType.DMA,
        ],
        compiler_params=pltpu.CompilerParams(vmem_limit_bytes=SPREAD_VMEM * 1024 * 1024),
        name="spread",
    )(*(pltpu.with_memory_space_constraint(v, pltpu.HBM) for v in (cells, owners, fx, fy, mass, live)))


def split(value):
    high = lax.reduce_precision(value, 8, 7)
    return high.astype(jnp.bfloat16), (value - high).astype(jnp.bfloat16)


def dft_parts():
    n = np.arange(NX)
    k = np.arange(32)
    coarse = 2.0 * np.pi / NX * ((32 * k[:, None] * n[None, :]) % NX)
    fine = 2.0 * np.pi / NX * ((k[:, None] * n[None, :]) % NX)
    return tuple(jnp.asarray(f(a), jnp.float32) for a in (coarse, fine) for f in (np.cos, np.sin))


def dft_tables():
    cc, cs, fc, fs = lax.optimization_barrier(dft_parts())
    cc, cs = cc[:, None, :], cs[:, None, :]
    fc, fs = fc[None, :, :], fs[None, :, :]
    cosine = (cc * fc - cs * fs).reshape(NX, NX)
    sine = (cs * fc + cc * fs).reshape(NX, NX)
    return split(cosine) + split(sine)


def dot(a, b):
    return jnp.dot(a, b, preferred_element_type=jnp.float32)


def power_of(top):
    return jnp.clip(jnp.floor(jnp.log2(jnp.maximum(top, 1e-30))) + 1.0, -90.0, 90.0).astype(jnp.int32)


def scale_of(power):
    return jnp.exp2((power - 15).astype(jnp.float32))


def coded_as(value, power):
    steps = jnp.round(value * jnp.exp2((15 - power).astype(jnp.float32)))
    return jnp.clip(steps, -32767.0, 32767.0).astype(jnp.int16)


def coded_rows(value, spare):
    power = power_of(jnp.max(jnp.abs(value), axis=-2, keepdims=True))
    row = lax.broadcasted_iota(jnp.int32, value.shape, value.ndim - 2)
    return jnp.where(row == spare, power.astype(jnp.int16), coded_as(value, power))


def plain_rows(coded, spare):
    power = lax.slice_in_dim(coded, spare, spare + 1, axis=coded.ndim - 2).astype(jnp.int32)
    row = lax.broadcasted_iota(jnp.int32, coded.shape, coded.ndim - 2)
    return jnp.where(row == spare, 0.0, coded.astype(jnp.float32) * scale_of(power))


def digits(value, width):
    power = power_of(value)
    scaled = value * jnp.exp2((14 - power).astype(jnp.float32))
    high = jnp.clip(jnp.floor(scaled), 0.0, 32767.0)
    low = jnp.clip(jnp.floor((scaled - high) * 16384.0), 0.0, 16384.0)
    lane = lax.broadcasted_iota(jnp.int32, (1, width), 1)
    rest = jnp.where(lane == 1, high, low).astype(jnp.int32)
    return jnp.where(lane == 0, power, rest)


def number(row):
    value = row[..., 1].astype(jnp.float32) + row[..., 2].astype(jnp.float32) / 16384.0
    return value * jnp.exp2((row[..., 0] - 14).astype(jnp.float32))


def scaled(out, total):
    py_count = lax.axis_size("py")
    ky_part = out.shape[2]
    norm = 1.0 / math.sqrt(NX * NY)
    index = lax.axis_index("px") * py_count + lax.axis_index("py")
    shape = (2, 1, ky_part, NX)
    at_zero = (
        (lax.broadcasted_iota(jnp.int32, shape, 0) == 0)
        & (lax.broadcasted_iota(jnp.int32, shape, 2) + index == 0)
        & (lax.broadcasted_iota(jnp.int32, shape, 3) == 0)
    )
    return out * (PLANES * NX * NY * norm / total) - jnp.where(at_zero, NX * NY * norm, 0.0)


def code_power(top):
    return jnp.clip(jnp.floor(jnp.log2(jnp.maximum(top, 1e-30))) + 1.0, -90.0, 90.0)


def code_block(read, store, row_groups, spare):
    top = None
    for r in range(row_groups):
        here = jnp.abs(read(r))
        top = here if top is None else jnp.maximum(top, here)
    power = code_power(jnp.max(top, axis=0, keepdims=True))
    factor = jnp.exp2(15.0 - power)
    for r in range(row_groups):
        steps = jnp.clip(jnp.round(read(r) * factor), -32767.0, 32767.0)
        if r == row_groups - 1 and spare is not None:
            row = lax.broadcasted_iota(jnp.int32, steps.shape, 0)
            steps = jnp.where(row == spare, power, steps)
        store(r, steps.astype(jnp.int32).astype(jnp.int16))
    return power


def exchange_kernel(px_count, py_count, grid_ref, counts_ref, coarse_c_in, coarse_s_in, fine_c_in,
                    fine_s_in, out_ref, starts_ref, factor_ref,
                    coarse_c_ref, coarse_s_ref, fine_c_ref, fine_s_ref, table_sems,
                    pair_ref, own_ref, code_ref, got_ref, zcode_ref, zgot_ref, edge_ref, dhl_ref,
                    chi_ref, clo_ref, shi_ref, slo_ref, fcode_ref, fgot_ref, lhs_ref, line_ref,
                    info_ref, infos_ref,
                    pair_send, pair_recv, code_send, code_recv, z_send, z_recv, f_send, f_recv,
                    i_send, i_recv):
    px = lax.axis_index("px")
    py = lax.axis_index("py")
    core = px % 2
    chip = px // 2
    chips = px_count // 2
    other = px + 1 - 2 * core
    blocks, tiles, height, _ = grid_ref.shape
    near = py_count // 2
    half = py // near
    seat = py % near
    part = tiles // near
    chunks = near * part
    col_count = height - 16
    groups = height // 16
    spare = 8
    width = part * LANES
    devices = px_count * py_count
    ky_part = NY // devices
    norm = 1.0 / math.sqrt(NX * NY)
    mesh_id = pl.DeviceIdType.MESH

    tables = [
        pltpu.make_async_copy(source, target, table_sems.at[k])
        for k, (source, target) in enumerate(
            (
                (coarse_c_in, coarse_c_ref),
                (coarse_s_in, coarse_s_ref),
                (fine_c_in, fine_c_ref),
                (fine_s_in, fine_s_ref),
            )
        )
    ]
    for copy in tables:
        copy.start()
    barrier = pltpu.get_barrier_semaphore()
    for e in range(2):
        for s in range(chips):
            for m in range(py_count):
                if e + s + m > 0:
                    to = ((chip + s) % chips * 2 + (core + e) % 2, (py + m) % py_count)
                    pl.semaphore_signal(barrier, inc=1, device_id=to, device_id_type=mesh_id)
    pl.semaphore_wait(barrier, devices - 1)

    def split_of(c):
        return near - 1 - c // part, c % part

    def tile_of(c):
        a, k = split_of(c)
        return (seat + a) % near * part + k

    def pair_copy(c, s):
        block = (chip + s) % chips * 2
        return pltpu.make_async_remote_copy(
            src_ref=grid_ref.at[block + 1 - core, tile_of(c)],
            dst_ref=pair_ref.at[c, s],
            send_sem=pair_send.at[c, s],
            recv_sem=pair_recv.at[c, s],
            device_id=(other, py),
            device_id_type=mesh_id,
        )

    def code_copy(c, s):
        return pltpu.make_async_remote_copy(
            src_ref=code_ref.at[c, s - 1],
            dst_ref=got_ref.at[c, s - 1],
            send_sem=code_send.at[c, s - 1],
            recv_sem=code_recv.at[c, s - 1],
            device_id=((chip + s) % chips * 2 + core, py),
            device_id_type=mesh_id,
        )

    def z_copy(a, k, b):
        return pltpu.make_async_remote_copy(
            src_ref=zcode_ref.at[a, k],
            dst_ref=zgot_ref.at[a, b, k],
            send_sem=z_send.at[a, b, k],
            recv_sem=z_recv.at[a, b, k],
            device_id=(px, (half + b) % 2 * near + (seat + a) % near),
            device_id_type=mesh_id,
        )

    def peer(s, e, a):
        return ((chip + s) % chips * 2 + (core + e) % 2, half * near + (seat + a) % near)

    def f_copy(s, e, a):
        return pltpu.make_async_remote_copy(
            src_ref=fcode_ref.at[s, e, a],
            dst_ref=fgot_ref.at[s, e, a],
            send_sem=f_send.at[s, e, a],
            recv_sem=f_recv.at[s, e, a],
            device_id=peer(s, e, a),
            device_id_type=mesh_id,
        )

    def i_copy(s, e, a):
        return pltpu.make_async_remote_copy(
            src_ref=info_ref,
            dst_ref=infos_ref.at[s, e, a],
            send_sem=i_send.at[s, e, a],
            recv_sem=i_recv.at[s, e, a],
            device_id=peer(s, e, a),
            device_id_type=mesh_id,
        )

    others = [(s, e, a) for s in range(chips) for e in range(2) for a in range(near) if s + e + a > 0]
    moves = [(a, b) for a in range(near - 1, -1, -1) for b in (1, 0) if a + b > 0]

    for c in range(chunks):
        for s in range(chips - 1, -1, -1):
            pair_copy(c, s).start()

    def add_pair(c):
        tile = tile_of(c)
        for s in range(chips - 1, -1, -1):
            pair_copy(c, s).wait_recv()
            block = (chip + s) % chips * 2 + core

            def summed(r):
                at = pl.ds(r * 16, 16)
                return grid_ref[block, tile, at, :] + pair_ref[c, s, at, :]

            if s == 0:
                for r in range(groups):
                    own_ref[c, pl.ds(r * 16, 16), :] = summed(r)
            else:
                def keep(r, value):
                    code_ref[c, s - 1, pl.ds(r * 16, 16), :] = value

                code_block(summed, keep, groups, spare)
                code_copy(c, s).start()

    def scale_in(rows):
        return jnp.exp2(rows.astype(jnp.int32)[spare : spare + 1].astype(jnp.float32) - 15.0)

    def plain(rows):
        return rows.astype(jnp.int32).astype(jnp.float32)

    row16 = lax.broadcasted_iota(jnp.int32, (16, LANES), 0)

    def gather(c):
        a, k = split_of(c)
        for s in range(chips - 1, 0, -1):
            code_copy(c, s).wait_recv()
        scales = [scale_in(got_ref[c, s, pl.ds(col_count, 16), :]) for s in range(chips - 1)]
        for r in range(groups):
            at = pl.ds(r * 16, 16)
            value = own_ref[c, at, :]
            for s in range(chips - 1):
                term = plain(got_ref[c, s, at, :]) * scales[s]
                if r == groups - 1:
                    term = jnp.where(row16 == spare, 0.0, term)
                value = value + term
            own_ref[c, at, :] = value

        def keep(r, value):
            zcode_ref[a, k, pl.ds(r * 16, 16), :] = value

        code_block(lambda r: own_ref[c, pl.ds(r * 16, 16), :], keep, groups, spare)
        for a2, b in moves:
            if a2 == a:
                z_copy(a, k, b).start()

    def make_tables():
        for copy in tables:
            copy.wait()

        def table(i, _):
            at = pl.ds(pl.multiple_of(i * 32, 32), 32)
            cc = coarse_c_ref[pl.ds(i, 1), :]
            cs = coarse_s_ref[pl.ds(i, 1), :]
            fc = fine_c_ref[...]
            fs = fine_s_ref[...]
            for value, high_ref, low_ref in (
                (cc * fc - cs * fs, chi_ref, clo_ref),
                (cs * fc + cc * fs, shi_ref, slo_ref),
            ):
                high = value.astype(jnp.bfloat16)
                high_ref[at, :] = high
                low_ref[at, :] = (value - high.astype(jnp.float32)).astype(jnp.bfloat16)
            return 0

        lax.fori_loop(0, NX // 32, table, 0)

    row8 = lax.broadcasted_iota(jnp.int32, (8, LANES), 0)

    def source_of(a, b):
        return (half + b) % 2 * near + (seat + near - a) % near

    def rows_in(a, b, k):
        if a + b == 0:
            return lambda r: own_ref[(near - 1) * part + k, pl.ds(r * 16, 16), :]
        scale = scale_in(zgot_ref[a, b, k, pl.ds(col_count, 16), :])
        return lambda r: plain(zgot_ref[a, b, k, pl.ds(r * 16, 16), :]) * scale

    def put_halves(row, cols, value):
        at = pl.ds(pl.multiple_of(row, 16), 16)
        high = value.astype(jnp.bfloat16)
        dhl_ref[0, at, cols] = high
        dhl_ref[1, at, cols] = (value - high.astype(jnp.float32)).astype(jnp.bfloat16)

    def place(a, b, k, total):
        if a + b > 0:
            z_copy(a, k, b).wait_recv()
        cols = pl.ds(k * LANES, LANES)
        source = source_of(a, b)
        rows = rows_in(a, b, k)
        for r in range(groups - 1):
            value = rows(r)
            total = total + value
            if r == 0:
                edge_ref[source, 0, :, cols] = value
            elif r == groups - 2:
                edge_ref[source, 1, :, cols] = value
            else:
                put_halves(source * col_count + r * 16, cols, value)
        return total

    def finish_rims(k, total):
        cols = pl.ds(k * LANES, LANES)
        for a, b in moves + [(0, 0)]:
            source = source_of(a, b)
            after = (source + 1) % py_count
            before = (source + py_count - 1) % py_count
            rim = rows_in(a, b, k)(groups - 1)
            first = jnp.where(row8 < 4, rim[:8], 0.0)
            second = jnp.where(row8 > 4, rim[8:], 0.0)
            edge_ref[after, 0, pl.ds(0, 8), cols] += first
            edge_ref[before, 1, pl.ds(8, 8), cols] += second
            total = total + jnp.concatenate([first, second], axis=0)
        for source in range(py_count):
            put_halves(source * col_count, cols, edge_ref[source, 0, :, cols])
            put_halves((source + 1) * col_count - 16, cols, edge_ref[source, 1, :, cols])
        return total

    lead = min(5, chunks)
    for c in range(lead):
        add_pair(c)
    gather(0)
    for c in range(lead, chunks):
        add_pair(c)
    total = jnp.zeros((16, LANES), jnp.float32)
    waiting = [(a, b, k) for a in range(near - 1, 0, -1) for k in range(part) for b in (1, 0)]
    for c in range(1, chunks):
        if c == min(3, chunks - 1):
            make_tables()
        gather(c)
        if c >= chunks - part:
            for _ in range(2):
                if waiting:
                    total = place(*waiting.pop(0), total)
    for k in range(part):
        total = place(0, 0, k, total)
    for a, b, k in waiting:
        total = place(a, b, k, total)
    for k in range(part):
        total = place(0, 1, k, total)
        total = finish_rims(k, total)
    total = jnp.sum(total)
    bucket_count = counts_ref.shape[1]
    info_ref[...] = jnp.where(row8 == 0, total, 0.0)
    info_ref[pl.ds(1, 1), pl.ds(0, bucket_count)] = counts_ref[...].astype(jnp.float32)
    for s, e, a in others:
        i_copy(s, e, a).start()

    span = near * ky_part

    def transform(s):
        def stack(cos_ref, sin_ref):
            rows = [
                pl.ds(pl.multiple_of((((chip + s) % chips * 2 + v) * py_count + half * near) * ky_part, span), span)
                for v in range(2)
            ]
            return jnp.concatenate([ref[at, :] for ref in (cos_ref, sin_ref) for at in rows], axis=0)

        high = stack(chi_ref, shi_ref)
        low = stack(clo_ref, slo_ref)
        for n in range(0, width, 256):
            cols = pl.ds(n, 256)
            both = jnp.dot(jnp.concatenate([high, low], axis=0), dhl_ref[0, :, cols],
                           preferred_element_type=jnp.float32)
            rest = jnp.dot(high, dhl_ref[1, :, cols], preferred_element_type=jnp.float32)
            line_ref[:, cols] = both[: 4 * span] + both[4 * span :] + rest
        row = lax.broadcasted_iota(jnp.int32, (8, width), 0)
        for e in range(2):
            for a in range(near):
                at = (core + e) % 2 * span + (seat + a) % near * ky_part
                real = line_ref[pl.ds(pl.multiple_of(at, ky_part), ky_part), :]
                imag = -line_ref[pl.ds(pl.multiple_of(2 * span + at, ky_part), ky_part), :]
                top = jnp.maximum(jnp.abs(real), jnp.abs(imag))
                power = code_power(jnp.max(top, axis=0, keepdims=True))
                factor = jnp.exp2(15.0 - power)
                for k, value in enumerate((real, imag)):
                    steps = jnp.clip(jnp.round(value * factor), -32767.0, 32767.0)
                    fcode_ref[s, e, a, pl.ds(k * ky_part, ky_part), :] = steps.astype(jnp.int32).astype(jnp.int16)
                rest = jnp.where(row == 0, power, 0.0)
                fcode_ref[s, e, a, pl.ds(2 * ky_part, 8), :] = rest.astype(jnp.int32).astype(jnp.int16)

    for s in SENDS:
        transform(s)
        for a in range(near - 1, -1, -1):
            for e in range(1, -1, -1):
                if s + e + a > 0:
                    f_copy(s, e, a).start()

    rows_all = px_count * ky_part
    quarter = 2 * ky_part

    def decode(s, e, a, ref):
        scale = jnp.exp2(plain(ref[s, e, a, pl.ds(2 * ky_part, 8), :])[0:1] - 15.0)
        cols = pl.ds(pl.multiple_of((seat + near - a) % near * width, width), width)
        for k in range(2):
            value = plain(ref[s, e, a, pl.ds(k * ky_part, ky_part), :]) * scale
            high = value.astype(jnp.bfloat16)
            at = k * quarter + e * ky_part
            lhs_ref[pl.ds(at, ky_part), cols] = high
            lhs_ref[pl.ds(2 * quarter + at, ky_part), cols] = (value - high.astype(jnp.float32)).astype(jnp.bfloat16)

    def finish(s):
        def some(n, _):
            cols = pl.ds(pl.multiple_of(n * WIDE, WIDE), WIDE)
            results = []
            for high_ref, low_ref in ((chi_ref, clo_ref), (shi_ref, slo_ref)):
                both = jnp.dot(lhs_ref[...], high_ref[:, cols], preferred_element_type=jnp.float32)
                rest = jnp.dot(lhs_ref[pl.ds(0, 2 * quarter), :], low_ref[:, cols], preferred_element_type=jnp.float32)
                results.append(both[: 2 * quarter] + both[2 * quarter :] + rest)
            by_cos, by_sin = results
            real = by_cos[:quarter] + by_sin[quarter:]
            imag = by_cos[quarter:] - by_sin[:quarter]
            for e in range(2):
                sender = (chip + chips - s) % chips * 2 + (core + e) % 2
                at = pl.multiple_of(sender * ky_part, ky_part)
                out_ref[pl.ds(at, ky_part), cols] = real[e * ky_part : (e + 1) * ky_part]
                out_ref[pl.ds(rows_all + at, ky_part), cols] = imag[e * ky_part : (e + 1) * ky_part]
            return 0

        lax.fori_loop(0, NX // WIDE, some, 0)

    for s in TAKES:
        for a in range(near):
            for e in range(2):
                if s + e + a == 0:
                    decode(s, e, a, fcode_ref)
                else:
                    f_copy(s, e, a).wait_recv()
                    decode(s, e, a, fgot_ref)
        finish(s)

    column = info_ref[pl.ds(1, 1), :]
    before = jnp.zeros((1, LANES), jnp.float32)
    sums = info_ref[...]
    for s, e, a in others:
        i_copy(s, e, a).wait_recv()
        info = infos_ref[s, e, a]
        sums = sums + info
        if a == 0:
            sender = (chip + chips - s) % chips * 2 + (core + e) % 2
            column = column + info[1:2]
            before = before + jnp.where(sender < px, info[1:2], 0.0)
    lane = lax.broadcasted_iota(jnp.int32, (1, LANES), 1)
    preceding = column
    step = 1
    while step < LANES:
        preceding = preceding + jnp.where(lane >= step, pltpu.roll(preceding, step, 1), 0.0)
        step *= 2
    begin = (preceding - column + before).astype(jnp.int32)
    starts_ref[0] = begin[:, :bucket_count]
    total = jnp.broadcast_to(sums[0:1, 0:1], (1, NX))
    factor_ref[0, 0] = (PLANES * NX * NY * norm) / total

    corner = (row8 == 0) & (lax.broadcasted_iota(jnp.int32, (8, LANES), 1) + px + py == 0)
    for plane in range(px_count):
        out_ref[pl.ds(plane * ky_part, 8), pl.ds(0, LANES)] -= jnp.where(corner, total[:, :LANES] / PLANES, 0.0)

    for c in range(chunks):
        for s in range(chips):
            pair_copy(c, s).wait_send()
            if s > 0:
                code_copy(c, s).wait_send()
    for a, b in moves:
        for k in range(part):
            z_copy(a, k, b).wait_send()
    for s, e, a in others:
        f_copy(s, e, a).wait_send()
        i_copy(s, e, a).wait_send()


def exchange(grid, counts, tables, px_count, py_count):
    blocks, tiles, height, _ = grid.shape
    chips = px_count // 2
    near = py_count // 2
    part = tiles // near
    chunks = near * part
    width = part * LANES
    col_count = height - 16
    ky_part = NY // (px_count * py_count)
    rows = px_count * ky_part
    vmem = pl.BlockSpec(memory_space=pltpu.VMEM)
    dma = pltpu.SemaphoreType.DMA
    f32, bf16, s16 = jnp.float32, jnp.bfloat16, jnp.int16
    return pl.pallas_call(
        functools.partial(exchange_kernel, px_count, py_count),
        out_shape=(
            jax.ShapeDtypeStruct((2 * rows, NX), f32),
            jax.ShapeDtypeStruct((1,) + counts.shape, jnp.int32),
            jax.ShapeDtypeStruct((1, 1, 1, NX), f32),
        ),
        in_specs=[vmem] * 2 + [pl.BlockSpec(memory_space=pltpu.HBM)] * 4,
        out_specs=[vmem] * 3,
        scratch_shapes=[pltpu.VMEM((32, NX), f32)] * 4
        + [
            dma((4,)),
            pltpu.VMEM((chunks, chips, height, LANES), f32),
            pltpu.VMEM((chunks, height, LANES), f32),
            pltpu.VMEM((chunks, chips - 1, height, LANES), s16),
            pltpu.VMEM((chunks, chips - 1, height, LANES), s16),
            pltpu.VMEM((near, part, height, LANES), s16),
            pltpu.VMEM((near, 2, part, height, LANES), s16),
            pltpu.VMEM((py_count, 2, 16, width), f32),
            pltpu.VMEM((2, NY, width), bf16),
        ]
        + [pltpu.VMEM((NX, NX), bf16)] * 4
        + [
            pltpu.VMEM((chips, 2, near, 2 * ky_part + 8, width), s16),
            pltpu.VMEM((chips, 2, near, 2 * ky_part + 8, width), s16),
            pltpu.VMEM((8 * ky_part, NX), bf16),
            pltpu.VMEM((4 * near * ky_part, width), f32),
            pltpu.VMEM((8, LANES), f32),
            pltpu.VMEM((chips, 2, near, 8, LANES), f32),
            dma((chunks, chips)),
            dma((chunks, chips)),
            dma((chunks, chips - 1)),
            dma((chunks, chips - 1)),
            dma((near, 2, part)),
            dma((near, 2, part)),
            dma((chips, 2, near)),
            dma((chips, 2, near)),
            dma((chips, 2, near)),
            dma((chips, 2, near)),
        ],
        compiler_params=pltpu.CompilerParams(
            collective_id=0, has_side_effects=True, vmem_limit_bytes=EXCHANGE_VMEM * 1024 * 1024
        ),
        name="exchange",
    )(grid, counts, *tables)


def local(cell_ids, offset_x, offset_y, mass, live, tile_owner, counts):
    px_count = lax.axis_size("px")
    py_count = lax.axis_size("py")
    row_count = NX // px_count
    col_count = NY // py_count
    parts = px_count // PLANES
    devices = px_count * py_count
    ky_part = NY // devices
    grid = spread(
        cell_ids[0], tile_owner, offset_x[0], offset_y[0], mass[0], live[0], row_count, col_count,
        px_count * PLANES,
    )
    bucket_count = counts.shape[-1]
    lane_tiles = NX // LANES
    if px_count == PLANES and py_count % 2 == 0 and lane_tiles % py_count == 0 and bucket_count <= LANES:
        out, begin, factor = exchange(grid, counts[0], dft_parts(), px_count, py_count)
        return (out.reshape(2, PLANES, ky_part, NX) * factor, begin)
    grid = grid.transpose(0, 2, 1, 3).reshape(PLANES, col_count + 16, NX)
    height = col_count + 16
    width = NX // parts
    if parts > 1:
        grid = grid.reshape(PLANES, height, parts, width).transpose(0, 2, 1, 3)
    grid = grid.reshape(px_count // 2, 2, height, width)
    side = lax.axis_index("px") % 2
    keep = lax.dynamic_index_in_dim(grid, side, 1, keepdims=False)
    away = lax.dynamic_index_in_dim(grid, 1 - side, 1, keepdims=False)
    pairs = [(source, source ^ 1) for source in range(px_count)]
    summed = keep + lax.ppermute(away, "px", pairs)
    groups = [list(range(k, px_count, 2)) for k in range(2)]
    got = lax.all_to_all(
        coded_rows(summed, col_count + 8), "px", 0, 0, axis_index_groups=groups, tiled=True
    )
    mine = jnp.sum(plain_rows(got, col_count + 8), axis=0)
    total = jnp.sum(mine)
    by_cols = lax.all_to_all(
        coded_rows(mine, col_count + 8), "py", split_axis=1, concat_axis=0, tiled=True
    )
    part = width // py_count
    ext = plain_rows(by_cols.reshape(py_count, height, part), col_count + 8)
    core = ext[:, :col_count]
    right = jnp.roll(ext[:, col_count : col_count + 4], 1, axis=0)
    left = jnp.roll(ext[:, col_count + 12 :], -1, axis=0)
    core = core + jnp.concatenate(
        [right, jnp.zeros((py_count, col_count - 8, part), jnp.float32), left], axis=1
    )
    data = core.reshape(NY, part)
    cos_hi, cos_lo, sin_hi, sin_lo = dft_tables()
    hi, lo = split(data)
    both = jnp.concatenate([hi, lo], axis=1)
    real = dot(cos_hi, both)
    real = real[:, :part] + real[:, part:] + dot(cos_lo, hi)
    imag = dot(sin_hi, both)
    imag = -(imag[:, :part] + imag[:, part:] + dot(sin_lo, hi))
    lines = jnp.stack([real.reshape(devices, ky_part, part), imag.reshape(devices, ky_part, part)], 1)
    lines = lines.reshape(devices, 2 * ky_part, part)
    power = power_of(jnp.max(jnp.abs(lines), axis=1, keepdims=True))
    coded = coded_as(lines, power)
    count_rows = -(-bucket_count // part)
    spare = -(2 + count_rows) % 8
    side_rows = jnp.concatenate(
        [
            digits(total, part),
            jnp.pad(counts.reshape(-1), (0, count_rows * part - bucket_count)).reshape(-1, part),
            jnp.zeros((spare, part), jnp.int32),
        ]
    ).astype(jnp.int16)
    side_rows = jnp.broadcast_to(side_rows[None], (devices,) + side_rows.shape)
    coded = jnp.concatenate([coded, power.astype(jnp.int16), side_rows], axis=1)
    got = lax.all_to_all(coded, ("px", "py"), split_axis=0, concat_axis=0, tiled=True)
    after = got[:, 2 * ky_part :].astype(jnp.int32)
    lines = got[:, : 2 * ky_part].astype(jnp.float32) * scale_of(after[:, :1])
    total = jnp.sum(number(after[:, 1]))
    column = after[:, 2 : 2 + count_rows].reshape(px_count, py_count, 1, count_rows * part)
    column = lax.dynamic_index_in_dim(column, lax.axis_index("py"), 1, keepdims=False)
    column = column[:, :, :bucket_count][:, None]
    got = lines.reshape(PLANES, parts * py_count, 2, ky_part, part).transpose(2, 0, 3, 1, 4)
    got = got.reshape(2 * PLANES * ky_part, NX)
    hi, lo = split(got)
    rows = PLANES * ky_part
    both = jnp.concatenate([hi, lo], axis=0)
    by_cos = dot(both, cos_hi)
    by_cos = by_cos[: 2 * rows] + by_cos[2 * rows :] + dot(hi, cos_lo)
    by_sin = dot(both, sin_hi)
    by_sin = by_sin[: 2 * rows] + by_sin[2 * rows :] + dot(hi, sin_lo)
    out = jnp.stack([by_cos[:rows] + by_sin[rows:], by_cos[rows:] - by_sin[:rows]])
    out = out.reshape(2, PLANES, ky_part, NX)
    spectrum = scaled(out, total)
    column_sum = jnp.sum(column, axis=0)
    reached = lax.broadcasted_iota(jnp.int32, column.shape, 0) < lax.axis_index("px")
    earlier = jnp.sum(jnp.where(reached, column, 0), axis=0)
    preceding = jnp.cumsum(column_sum, axis=-1) - column_sum
    bucket_start = (preceding + earlier).astype(jnp.int32)
    return (spectrum, bucket_start)


def solution(mesh):
    placed = (
        P("px", "py", None),
        P("px", "py", None),
        P("px", "py", None),
        P("px", "py", None),
        P("px", "py", None),
        P("px", "py"),
        P("px", "py", None),
    )
    return jax.shard_map(
        local,
        mesh=mesh,
        in_specs=placed,
        out_specs=(P(None, None, ("px", "py"), None), P("px", "py", None)),
        check_vma=False,
    )
```

```python
import functools
import math

import jax
import jax.numpy as jnp
import numpy as np
from jax import lax
from jax.experimental import pallas as pl
from jax.experimental.pallas import tpu as pltpu
from jax.sharding import PartitionSpec as P

NX = 1024
NY = 1024
PLANES = 8
BETA = 18.4
LANES = 128
GROUP = 4
UNROLL = 8
EAGER = 3
SPREAD_VMEM = 24
EXCHANGE_VMEM = 38
WIDE = 256
SENDS = (3, 2, 1, 0)
TAKES = (3, 0, 1, 2)
RATE = BETA / math.log(2.0)


def tap_blocks(start, fraction, scaling, rows):
    depth = (rows - start + 3) & 7
    z = ((depth - 3).astype(jnp.float32) - fraction) * 0.25
    u = jnp.maximum(1.0 - z * z, 0.0)
    taps = jnp.exp2(u * lax.rsqrt(jnp.maximum(u, 1e-30)) * RATE - RATE)
    if scaling is not None:
        taps = taps * scaling
    at = start - 3 + depth
    odd = (at & 8) != 0
    zero = jnp.zeros_like(taps)
    both = jnp.concatenate(
        [jnp.where(odd, zero, taps), jnp.where(odd, taps, zero)], axis=0
    ).astype(jnp.bfloat16)
    return both, at >> 4


def placed_blocks(taps, block, count):
    block = jnp.where(block < 0, count, block)
    block = jnp.concatenate([block, block], axis=0).astype(jnp.int16)
    none = jnp.zeros_like(taps)
    return [jnp.where(block == k, taps, none) for k in range(count + 1)]


def spread_kernel(row_count, col_count, bucket_count, cell_in, owner_in, fx_in, fy_in, mass_in, live_in,
                  out_ref, rim_ref, owner_ref, x_ref, y_ref, w_ref, c_ref, fx_ref, fy_ref, mass_ref, live_ref,
                  edge_ref, starts_ref, item_ref, sems, edge_sem):
    tiles = cell_in.shape[0]
    col_blocks = col_count // 16
    lane_tiles = NX // LANES
    owners_tile = LANES // row_count if row_count < LANES else 1
    height = col_count + 16
    rows = lax.broadcasted_iota(jnp.int32, (8, LANES), 0)
    spare = pl.ds(tiles, 8)
    copies = [
        pltpu.make_async_copy(source, target, sems.at[k])
        for k, (source, target) in enumerate(
            (
                (cell_in, c_ref.at[pl.ds(0, tiles)]),
                (owner_in, owner_ref),
                (fx_in, fx_ref),
                (fy_in, fy_ref),
                (mass_in, mass_ref),
                (live_in, live_ref),
            )
        )
    ]
    for copy in copies:
        copy.start()
    for ref in (x_ref, y_ref, w_ref, c_ref):
        ref[spare, :] = jnp.zeros((8, LANES), ref.dtype)
    rim_ref[...] = jnp.zeros_like(rim_ref)

    copies[0].wait()
    copies[1].wait()
    plane_bits = (row_count * col_count).bit_length() - 1
    groups = edge_ref.shape[0]
    for g in range(groups):
        edge = lax.broadcasted_iota(jnp.int32, (LANES, LANES), 1) + g * LANES
        found = jnp.zeros((8, LANES), jnp.int32)
        for k in range(0, tiles, LANES):
            count = min(LANES, tiles - k)
            owner = jnp.broadcast_to(owner_ref[:, pl.ds(k, LANES)], (LANES, LANES)).T
            bucket = owner[:count] * PLANES + lax.shift_right_logical(
                c_ref[pl.ds(k, count), :], plane_bits
            )
            lower = jnp.where(bucket < edge[:count], 1, 0)
            for r in range(0, count, 8):
                found = found + lower[r : r + 8]
        edge_ref[pl.ds(g, 1), :] = jnp.sum(found, axis=0, keepdims=True)
    edges = pltpu.make_async_copy(edge_ref, starts_ref, edge_sem)
    edges.start()
    out_ref[...] = jnp.zeros_like(out_ref)
    for copy in copies[2:]:
        copy.wait()
    x_ref[pl.ds(0, tiles), :] = fx_ref[...].astype(jnp.float32)
    y_ref[pl.ds(0, tiles), :] = fy_ref[...].astype(jnp.float32)
    mass = mass_ref[...].astype(jnp.float32)
    w_ref[pl.ds(0, tiles), :] = jnp.where(live_ref[...] == 1, mass, jnp.zeros_like(mass))
    edges.wait()

    def start_of(b):
        return starts_ref[lax.shift_right_logical(b, 7), b & (LANES - 1)]

    def of_bucket(b, at):
        begin = start_of(b)
        count = (start_of(b + 1) - begin + GROUP - 1) // GROUP
        word = b * 65536 + begin
        for c in range(EAGER):
            item_ref[at + c] = word + c * GROUP

        @pl.when(count > EAGER)
        def _():
            def one(c, _):
                item_ref[at + c] = word + c * GROUP
                return 0

            lax.fori_loop(EAGER, count, one, 0)

        return at + count

    items = lax.fori_loop(0, bucket_count, of_bucket, 0, unroll=4)
    for k in range(UNROLL):
        item_ref[items + k] = (bucket_count - 1) * 65536 + tiles

    def product(k):
        begin = item_ref[k] & 65535
        bucket = lax.shift_right_logical(item_ref[k], 16)
        end = start_of(bucket + 1)
        shift = bucket // PLANES % owners_tile * row_count
        wxs, wys = [], []
        for g in range(GROUP):
            t = begin + g
            at = pl.ds(t, 1)
            scale = jnp.where(t < end, 1.0, 0.0)
            cell = jnp.broadcast_to(c_ref[at, :], (8, LANES))
            lx = lax.shift_right_logical(cell, col_count.bit_length() - 1) & (row_count - 1)
            if owners_tile > 1:
                lx = lx + shift
            taps, block = tap_blocks(lx, x_ref[at, :], None, rows)
            wxs.append(jnp.concatenate(placed_blocks(taps, block, LANES // 16), axis=0))
            taps, block = tap_blocks(cell & (col_count - 1), y_ref[at, :], w_ref[at, :] * scale, rows)
            wys.append(jnp.concatenate(placed_blocks(taps, block, col_blocks), axis=0))
        return lax.dot_general(
            jnp.concatenate(wys, axis=1), jnp.concatenate(wxs, axis=1),
            (((1,), (1,)), ((), ())), preferred_element_type=jnp.float32
        )

    def some(i, _):
        results = [product(i * UNROLL + u) for u in range(UNROLL)]
        for u, result in enumerate(results):
            b = lax.shift_right_logical(item_ref[i * UNROLL + u], 16)
            plane = b % PLANES
            tile = (b // PLANES * row_count) // LANES
            out_ref[plane, tile] += result[:, :LANES]
            rim_ref[plane, tile] += jnp.concatenate(
                [result[:, LANES:], jnp.zeros((height, LANES - 16), jnp.float32)], axis=1
            )
        return 0

    lax.fori_loop(0, (items + UNROLL - 1) // UNROLL, some, 0)

    lane = lax.broadcasted_iota(jnp.int32, (8, LANES), 1)

    def close(i, _):
        plane = i
        for tile in range(lane_tiles):
            low = (tile + lane_tiles - 1) % lane_tiles
            high = (tile + 1) % lane_tiles
            for r in range(0, height, 8):
                at = pl.ds(r, 8)
                left = jnp.where(lane < 8, rim_ref[plane, low, at, :], 0.0)
                right = jnp.where(lane < 8, 0.0, rim_ref[plane, high, at, :])
                out_ref[plane, tile, at, :] += left + pltpu.roll(right, LANES - 16, 1)
        return 0

    lax.fori_loop(0, PLANES, close, 0)


def spread(cells, owners, fx, fy, mass, live, row_count, col_count, bucket_count):
    height = col_count + 16
    tiles = cells.shape[0]
    vmem = pl.BlockSpec(memory_space=pltpu.VMEM)
    anywhere = pl.BlockSpec(memory_space=pltpu.HBM)
    wide = -(-tiles // LANES) * LANES
    owners = jnp.pad(owners, ((0, 0), (0, wide - tiles)))
    edges = (-(-(bucket_count + 1) // LANES), LANES)
    return pl.pallas_call(
        functools.partial(spread_kernel, row_count, col_count, bucket_count),
        out_shape=jax.ShapeDtypeStruct((PLANES, NX // LANES, height, LANES), jnp.float32),
        in_specs=[anywhere] * 6,
        out_specs=vmem,
        scratch_shapes=[
            pltpu.VMEM((PLANES, NX // LANES, height, LANES), jnp.float32),
            pltpu.VMEM((1, wide), jnp.int32),
            pltpu.VMEM((tiles + 8, LANES), jnp.float32),
            pltpu.VMEM((tiles + 8, LANES), jnp.float32),
            pltpu.VMEM((tiles + 8, LANES), jnp.float32),
            pltpu.VMEM((tiles + 8, LANES), jnp.int32),
            pltpu.VMEM((tiles, LANES), fx.dtype),
            pltpu.VMEM((tiles, LANES), fy.dtype),
            pltpu.VMEM((tiles, LANES), mass.dtype),
            pltpu.VMEM((tiles, LANES), live.dtype),
            pltpu.VMEM(edges, jnp.int32),
            pltpu.SMEM(edges, jnp.int32),
            pltpu.SMEM((-(-tiles // GROUP) + bucket_count + UNROLL + EAGER,), jnp.int32),
            pltpu.SemaphoreType.DMA((6,)),
            pltpu.SemaphoreType.DMA,
        ],
        compiler_params=pltpu.CompilerParams(vmem_limit_bytes=SPREAD_VMEM * 1024 * 1024),
        name="spread",
    )(*(pltpu.with_memory_space_constraint(v, pltpu.HBM) for v in (cells, owners, fx, fy, mass, live)))


def split(value):
    high = lax.reduce_precision(value, 8, 7)
    return high.astype(jnp.bfloat16), (value - high).astype(jnp.bfloat16)


def dft_parts():
    n = np.arange(NX)
    k = np.arange(32)
    coarse = 2.0 * np.pi / NX * ((32 * k[:, None] * n[None, :]) % NX)
    fine = 2.0 * np.pi / NX * ((k[:, None] * n[None, :]) % NX)
    return tuple(jnp.asarray(f(a), jnp.float32) for a in (coarse, fine) for f in (np.cos, np.sin))


def dft_tables():
    cc, cs, fc, fs = lax.optimization_barrier(dft_parts())
    cc, cs = cc[:, None, :], cs[:, None, :]
    fc, fs = fc[None, :, :], fs[None, :, :]
    cosine = (cc * fc - cs * fs).reshape(NX, NX)
    sine = (cs * fc + cc * fs).reshape(NX, NX)
    return split(cosine) + split(sine)


def dot(a, b):
    return jnp.dot(a, b, preferred_element_type=jnp.float32)


def power_of(top):
    return jnp.clip(jnp.floor(jnp.log2(jnp.maximum(top, 1e-30))) + 1.0, -90.0, 90.0).astype(jnp.int32)


def scale_of(power):
    return jnp.exp2((power - 15).astype(jnp.float32))


def coded_as(value, power):
    steps = jnp.round(value * jnp.exp2((15 - power).astype(jnp.float32)))
    return jnp.clip(steps, -32767.0, 32767.0).astype(jnp.int16)


def coded_rows(value, spare):
    power = power_of(jnp.max(jnp.abs(value), axis=-2, keepdims=True))
    row = lax.broadcasted_iota(jnp.int32, value.shape, value.ndim - 2)
    return jnp.where(row == spare, power.astype(jnp.int16), coded_as(value, power))


def plain_rows(coded, spare):
    power = lax.slice_in_dim(coded, spare, spare + 1, axis=coded.ndim - 2).astype(jnp.int32)
    row = lax.broadcasted_iota(jnp.int32, coded.shape, coded.ndim - 2)
    return jnp.where(row == spare, 0.0, coded.astype(jnp.float32) * scale_of(power))


def digits(value, width):
    power = power_of(value)
    scaled = value * jnp.exp2((14 - power).astype(jnp.float32))
    high = jnp.clip(jnp.floor(scaled), 0.0, 32767.0)
    low = jnp.clip(jnp.floor((scaled - high) * 16384.0), 0.0, 16384.0)
    lane = lax.broadcasted_iota(jnp.int32, (1, width), 1)
    rest = jnp.where(lane == 1, high, low).astype(jnp.int32)
    return jnp.where(lane == 0, power, rest)


def number(row):
    value = row[..., 1].astype(jnp.float32) + row[..., 2].astype(jnp.float32) / 16384.0
    return value * jnp.exp2((row[..., 0] - 14).astype(jnp.float32))


def scaled(out, total):
    py_count = lax.axis_size("py")
    ky_part = out.shape[2]
    norm = 1.0 / math.sqrt(NX * NY)
    index = lax.axis_index("px") * py_count + lax.axis_index("py")
    shape = (2, 1, ky_part, NX)
    at_zero = (
        (lax.broadcasted_iota(jnp.int32, shape, 0) == 0)
        & (lax.broadcasted_iota(jnp.int32, shape, 2) + index == 0)
        & (lax.broadcasted_iota(jnp.int32, shape, 3) == 0)
    )
    return out * (PLANES * NX * NY * norm / total) - jnp.where(at_zero, NX * NY * norm, 0.0)


def code_power(top):
    return jnp.clip(jnp.floor(jnp.log2(jnp.maximum(top, 1e-30))) + 1.0, -90.0, 90.0)


def code_block(read, store, row_groups, spare):
    top = None
    for r in range(row_groups):
        here = jnp.abs(read(r))
        top = here if top is None else jnp.maximum(top, here)
    power = code_power(jnp.max(top, axis=0, keepdims=True))
    factor = jnp.exp2(15.0 - power)
    for r in range(row_groups):
        steps = jnp.clip(jnp.round(read(r) * factor), -32767.0, 32767.0)
        if r == row_groups - 1 and spare is not None:
            row = lax.broadcasted_iota(jnp.int32, steps.shape, 0)
            steps = jnp.where(row == spare, power, steps)
        store(r, steps.astype(jnp.int32).astype(jnp.int16))
    return power


def exchange_kernel(px_count, py_count, grid_ref, counts_ref, coarse_c_in, coarse_s_in, fine_c_in,
                    fine_s_in, out_ref, starts_ref, factor_ref,
                    coarse_c_ref, coarse_s_ref, fine_c_ref, fine_s_ref, table_sems,
                    pair_ref, own_ref, code_ref, got_ref, zcode_ref, zgot_ref, edge_ref, dhl_ref,
                    chi_ref, clo_ref, shi_ref, slo_ref, fcode_ref, fgot_ref, lhs_ref, line_ref,
                    info_ref, infos_ref,
                    pair_send, pair_recv, code_send, code_recv, z_send, z_recv, f_send, f_recv,
                    i_send, i_recv):
    px = lax.axis_index("px")
    py = lax.axis_index("py")
    core = px % 2
    chip = px // 2
    chips = px_count // 2
    other = px + 1 - 2 * core
    blocks, tiles, height, _ = grid_ref.shape
    near = py_count // 2
    half = py // near
    seat = py % near
    part = tiles // near
    chunks = near * part
    col_count = height - 16
    groups = height // 16
    spare = 8
    width = part * LANES
    devices = px_count * py_count
    ky_part = NY // devices
    norm = 1.0 / math.sqrt(NX * NY)
    mesh_id = pl.DeviceIdType.MESH

    tables = [
        pltpu.make_async_copy(source, target, table_sems.at[k])
        for k, (source, target) in enumerate(
            (
                (coarse_c_in, coarse_c_ref),
                (coarse_s_in, coarse_s_ref),
                (fine_c_in, fine_c_ref),
                (fine_s_in, fine_s_ref),
            )
        )
    ]
    for copy in tables:
        copy.start()
    barrier = pltpu.get_barrier_semaphore()
    for e in range(2):
        for s in range(chips):
            for m in range(py_count):
                if e + s + m > 0:
                    to = ((chip + s) % chips * 2 + (core + e) % 2, (py + m) % py_count)
                    pl.semaphore_signal(barrier, inc=1, device_id=to, device_id_type=mesh_id)
    pl.semaphore_wait(barrier, devices - 1)

    def split_of(c):
        return near - 1 - c // part, c % part

    def tile_of(c):
        a, k = split_of(c)
        return (seat + a) % near * part + k

    def pair_copy(c, s):
        block = (chip + s) % chips * 2
        return pltpu.make_async_remote_copy(
            src_ref=grid_ref.at[block + 1 - core, tile_of(c)],
            dst_ref=pair_ref.at[c, s],
            send_sem=pair_send.at[c, s],
            recv_sem=pair_recv.at[c, s],
            device_id=(other, py),
            device_id_type=mesh_id,
        )

    def code_copy(c, s):
        return pltpu.make_async_remote_copy(
            src_ref=code_ref.at[c, s - 1],
            dst_ref=got_ref.at[c, s - 1],
            send_sem=code_send.at[c, s - 1],
            recv_sem=code_recv.at[c, s - 1],
            device_id=((chip + s) % chips * 2 + core, py),
            device_id_type=mesh_id,
        )

    def z_copy(a, k, b):
        return pltpu.make_async_remote_copy(
            src_ref=zcode_ref.at[a, k],
            dst_ref=zgot_ref.at[a, b, k],
            send_sem=z_send.at[a, b, k],
            recv_sem=z_recv.at[a, b, k],
            device_id=(px, (half + b) % 2 * near + (seat + a) % near),
            device_id_type=mesh_id,
        )

    def peer(s, e, a):
        return ((chip + s) % chips * 2 + (core + e) % 2, half * near + (seat + a) % near)

    def f_copy(s, e, a):
        return pltpu.make_async_remote_copy(
            src_ref=fcode_ref.at[s, e, a],
            dst_ref=fgot_ref.at[s, e, a],
            send_sem=f_send.at[s, e, a],
            recv_sem=f_recv.at[s, e, a],
            device_id=peer(s, e, a),
            device_id_type=mesh_id,
        )

    def i_copy(s, e, a):
        return pltpu.make_async_remote_copy(
            src_ref=info_ref,
            dst_ref=infos_ref.at[s, e, a],
            send_sem=i_send.at[s, e, a],
            recv_sem=i_recv.at[s, e, a],
            device_id=peer(s, e, a),
            device_id_type=mesh_id,
        )

    others = [(s, e, a) for s in range(chips) for e in range(2) for a in range(near) if s + e + a > 0]
    moves = [(a, b) for a in range(near - 1, -1, -1) for b in (1, 0) if a + b > 0]

    for c in range(chunks):
        for s in range(chips - 1, -1, -1):
            pair_copy(c, s).start()

    def add_pair(c):
        tile = tile_of(c)
        for s in range(chips - 1, -1, -1):
            pair_copy(c, s).wait_recv()
            block = (chip + s) % chips * 2 + core

            def summed(r):
                at = pl.ds(r * 16, 16)
                return grid_ref[block, tile, at, :] + pair_ref[c, s, at, :]

            if s == 0:
                for r in range(groups):
                    own_ref[c, pl.ds(r * 16, 16), :] = summed(r)
            else:
                def keep(r, value):
                    code_ref[c, s - 1, pl.ds(r * 16, 16), :] = value

                code_block(summed, keep, groups, spare)
                code_copy(c, s).start()

    def scale_in(rows):
        return jnp.exp2(rows.astype(jnp.int32)[spare : spare + 1].astype(jnp.float32) - 15.0)

    def plain(rows):
        return rows.astype(jnp.int32).astype(jnp.float32)

    row16 = lax.broadcasted_iota(jnp.int32, (16, LANES), 0)

    def gather(c):
        a, k = split_of(c)
        for s in range(chips - 1, 0, -1):
            code_copy(c, s).wait_recv()
        scales = [scale_in(got_ref[c, s, pl.ds(col_count, 16), :]) for s in range(chips - 1)]
        for r in range(groups):
            at = pl.ds(r * 16, 16)
            value = own_ref[c, at, :]
            for s in range(chips - 1):
                term = plain(got_ref[c, s, at, :]) * scales[s]
                if r == groups - 1:
                    term = jnp.where(row16 == spare, 0.0, term)
                value = value + term
            own_ref[c, at, :] = value

        def keep(r, value):
            zcode_ref[a, k, pl.ds(r * 16, 16), :] = value

        code_block(lambda r: own_ref[c, pl.ds(r * 16, 16), :], keep, groups, spare)
        for a2, b in moves:
            if a2 == a:
                z_copy(a, k, b).start()

    def make_tables():
        for copy in tables:
            copy.wait()

        def table(i, _):
            at = pl.ds(pl.multiple_of(i * 32, 32), 32)
            cc = coarse_c_ref[pl.ds(i, 1), :]
            cs = coarse_s_ref[pl.ds(i, 1), :]
            fc = fine_c_ref[...]
            fs = fine_s_ref[...]
            for value, high_ref, low_ref in (
                (cc * fc - cs * fs, chi_ref, clo_ref),
                (cs * fc + cc * fs, shi_ref, slo_ref),
            ):
                high = value.astype(jnp.bfloat16)
                high_ref[at, :] = high
                low_ref[at, :] = (value - high.astype(jnp.float32)).astype(jnp.bfloat16)
            return 0

        lax.fori_loop(0, NX // 32, table, 0)

    row8 = lax.broadcasted_iota(jnp.int32, (8, LANES), 0)

    def source_of(a, b):
        return (half + b) % 2 * near + (seat + near - a) % near

    def rows_in(a, b, k):
        if a + b == 0:
            return lambda r: own_ref[(near - 1) * part + k, pl.ds(r * 16, 16), :]
        scale = scale_in(zgot_ref[a, b, k, pl.ds(col_count, 16), :])
        return lambda r: plain(zgot_ref[a, b, k, pl.ds(r * 16, 16), :]) * scale

    def put_halves(row, cols, value):
        at = pl.ds(pl.multiple_of(row, 16), 16)
        high = value.astype(jnp.bfloat16)
        dhl_ref[0, at, cols] = high
        dhl_ref[1, at, cols] = (value - high.astype(jnp.float32)).astype(jnp.bfloat16)

    def place(a, b, k, total):
        if a + b > 0:
            z_copy(a, k, b).wait_recv()
        cols = pl.ds(k * LANES, LANES)
        source = source_of(a, b)
        rows = rows_in(a, b, k)
        for r in range(groups - 1):
            value = rows(r)
            total = total + value
            if r == 0:
                edge_ref[source, 0, :, cols] = value
            elif r == groups - 2:
                edge_ref[source, 1, :, cols] = value
            else:
                put_halves(source * col_count + r * 16, cols, value)
        return total

    def finish_rims(k, total):
        cols = pl.ds(k * LANES, LANES)
        for a, b in moves + [(0, 0)]:
            source = source_of(a, b)
            after = (source + 1) % py_count
            before = (source + py_count - 1) % py_count
            rim = rows_in(a, b, k)(groups - 1)
            first = jnp.where(row8 < 4, rim[:8], 0.0)
            second = jnp.where(row8 > 4, rim[8:], 0.0)
            edge_ref[after, 0, pl.ds(0, 8), cols] += first
            edge_ref[before, 1, pl.ds(8, 8), cols] += second
            total = total + jnp.concatenate([first, second], axis=0)
        for source in range(py_count):
            put_halves(source * col_count, cols, edge_ref[source, 0, :, cols])
            put_halves((source + 1) * col_count - 16, cols, edge_ref[source, 1, :, cols])
        return total

    lead = min(5, chunks)
    for c in range(lead):
        add_pair(c)
    gather(0)
    for c in range(lead, chunks):
        add_pair(c)
    total = jnp.zeros((16, LANES), jnp.float32)
    waiting = [(a, b, k) for a in range(near - 1, 0, -1) for k in range(part) for b in (1, 0)]
    for c in range(1, chunks):
        if c == min(3, chunks - 1):
            make_tables()
        gather(c)
        if c >= chunks - part:
            for _ in range(2):
                if waiting:
                    total = place(*waiting.pop(0), total)
    for k in range(part):
        total = place(0, 0, k, total)
    for a, b, k in waiting:
        total = place(a, b, k, total)
    for k in range(part):
        total = place(0, 1, k, total)
        total = finish_rims(k, total)
    total = jnp.sum(total)
    bucket_count = counts_ref.shape[1]
    info_ref[...] = jnp.where(row8 == 0, total, 0.0)
    info_ref[pl.ds(1, 1), pl.ds(0, bucket_count)] = counts_ref[...].astype(jnp.float32)
    for s, e, a in others:
        i_copy(s, e, a).start()

    span = near * ky_part

    def transform(s):
        def stack(cos_ref, sin_ref):
            rows = [
                pl.ds(pl.multiple_of((((chip + s) % chips * 2 + v) * py_count + half * near) * ky_part, span), span)
                for v in range(2)
            ]
            return jnp.concatenate([ref[at, :] for ref in (cos_ref, sin_ref) for at in rows], axis=0)

        high = stack(chi_ref, shi_ref)
        low = stack(clo_ref, slo_ref)
        for n in range(0, width, 256):
            cols = pl.ds(n, 256)
            both = jnp.dot(jnp.concatenate([high, low], axis=0), dhl_ref[0, :, cols],
                           preferred_element_type=jnp.float32)
            rest = jnp.dot(high, dhl_ref[1, :, cols], preferred_element_type=jnp.float32)
            line_ref[:, cols] = both[: 4 * span] + both[4 * span :] + rest
        row = lax.broadcasted_iota(jnp.int32, (8, width), 0)
        for e in range(2):
            for a in range(near):
                at = (core + e) % 2 * span + (seat + a) % near * ky_part
                real = line_ref[pl.ds(pl.multiple_of(at, ky_part), ky_part), :]
                imag = -line_ref[pl.ds(pl.multiple_of(2 * span + at, ky_part), ky_part), :]
                top = jnp.maximum(jnp.abs(real), jnp.abs(imag))
                power = code_power(jnp.max(top, axis=0, keepdims=True))
                factor = jnp.exp2(15.0 - power)
                for k, value in enumerate((real, imag)):
                    steps = jnp.clip(jnp.round(value * factor), -32767.0, 32767.0)
                    fcode_ref[s, e, a, pl.ds(k * ky_part, ky_part), :] = steps.astype(jnp.int32).astype(jnp.int16)
                rest = jnp.where(row == 0, power, 0.0)
                fcode_ref[s, e, a, pl.ds(2 * ky_part, 8), :] = rest.astype(jnp.int32).astype(jnp.int16)

    for s in SENDS:
        transform(s)
        for a in range(near - 1, -1, -1):
            for e in range(1, -1, -1):
                if s + e + a > 0:
                    f_copy(s, e, a).start()

    rows_all = px_count * ky_part
    quarter = 2 * ky_part

    def decode(s, e, a, ref):
        scale = jnp.exp2(plain(ref[s, e, a, pl.ds(2 * ky_part, 8), :])[0:1] - 15.0)
        cols = pl.ds(pl.multiple_of((seat + near - a) % near * width, width), width)
        for k in range(2):
            value = plain(ref[s, e, a, pl.ds(k * ky_part, ky_part), :]) * scale
            high = value.astype(jnp.bfloat16)
            at = k * quarter + e * ky_part
            lhs_ref[pl.ds(at, ky_part), cols] = high
            lhs_ref[pl.ds(2 * quarter + at, ky_part), cols] = (value - high.astype(jnp.float32)).astype(jnp.bfloat16)

    def finish(s):
        def some(n, _):
            cols = pl.ds(pl.multiple_of(n * WIDE, WIDE), WIDE)
            results = []
            for high_ref, low_ref in ((chi_ref, clo_ref), (shi_ref, slo_ref)):
                both = jnp.dot(lhs_ref[...], high_ref[:, cols], preferred_element_type=jnp.float32)
                rest = jnp.dot(lhs_ref[pl.ds(0, 2 * quarter), :], low_ref[:, cols], preferred_element_type=jnp.float32)
                results.append(both[: 2 * quarter] + both[2 * quarter :] + rest)
            by_cos, by_sin = results
            real = by_cos[:quarter] + by_sin[quarter:]
            imag = by_cos[quarter:] - by_sin[:quarter]
            for e in range(2):
                sender = (chip + chips - s) % chips * 2 + (core + e) % 2
                at = pl.multiple_of(sender * ky_part, ky_part)
                out_ref[pl.ds(at, ky_part), cols] = real[e * ky_part : (e + 1) * ky_part]
                out_ref[pl.ds(rows_all + at, ky_part), cols] = imag[e * ky_part : (e + 1) * ky_part]
            return 0

        lax.fori_loop(0, NX // WIDE, some, 0)

    for s in TAKES:
        for a in range(near):
            for e in range(2):
                if s + e + a == 0:
                    decode(s, e, a, fcode_ref)
                else:
                    f_copy(s, e, a).wait_recv()
                    decode(s, e, a, fgot_ref)
        finish(s)

    column = info_ref[pl.ds(1, 1), :]
    before = jnp.zeros((1, LANES), jnp.float32)
    sums = info_ref[...]
    for s, e, a in others:
        i_copy(s, e, a).wait_recv()
        info = infos_ref[s, e, a]
        sums = sums + info
        if a == 0:
            sender = (chip + chips - s) % chips * 2 + (core + e) % 2
            column = column + info[1:2]
            before = before + jnp.where(sender < px, info[1:2], 0.0)
    lane = lax.broadcasted_iota(jnp.int32, (1, LANES), 1)
    preceding = column
    step = 1
    while step < LANES:
        preceding = preceding + jnp.where(lane >= step, pltpu.roll(preceding, step, 1), 0.0)
        step *= 2
    begin = (preceding - column + before).astype(jnp.int32)
    starts_ref[0] = begin[:, :bucket_count]
    total = jnp.broadcast_to(sums[0:1, 0:1], (1, NX))
    factor_ref[0, 0] = (PLANES * NX * NY * norm) / total

    corner = (row8 == 0) & (lax.broadcasted_iota(jnp.int32, (8, LANES), 1) + px + py == 0)
    for plane in range(px_count):
        out_ref[pl.ds(plane * ky_part, 8), pl.ds(0, LANES)] -= jnp.where(corner, total[:, :LANES] / PLANES, 0.0)

    for c in range(chunks):
        for s in range(chips):
            pair_copy(c, s).wait_send()
            if s > 0:
                code_copy(c, s).wait_send()
    for a, b in moves:
        for k in range(part):
            z_copy(a, k, b).wait_send()
    for s, e, a in others:
        f_copy(s, e, a).wait_send()
        i_copy(s, e, a).wait_send()


def exchange(grid, counts, tables, px_count, py_count):
    blocks, tiles, height, _ = grid.shape
    chips = px_count // 2
    near = py_count // 2
    part = tiles // near
    chunks = near * part
    width = part * LANES
    col_count = height - 16
    ky_part = NY // (px_count * py_count)
    rows = px_count * ky_part
    vmem = pl.BlockSpec(memory_space=pltpu.VMEM)
    dma = pltpu.SemaphoreType.DMA
    f32, bf16, s16 = jnp.float32, jnp.bfloat16, jnp.int16
    return pl.pallas_call(
        functools.partial(exchange_kernel, px_count, py_count),
        out_shape=(
            jax.ShapeDtypeStruct((2 * rows, NX), f32),
            jax.ShapeDtypeStruct((1,) + counts.shape, jnp.int32),
            jax.ShapeDtypeStruct((1, 1, 1, NX), f32),
        ),
        in_specs=[vmem] * 2 + [pl.BlockSpec(memory_space=pltpu.HBM)] * 4,
        out_specs=[vmem] * 3,
        scratch_shapes=[pltpu.VMEM((32, NX), f32)] * 4
        + [
            dma((4,)),
            pltpu.VMEM((chunks, chips, height, LANES), f32),
            pltpu.VMEM((chunks, height, LANES), f32),
            pltpu.VMEM((chunks, chips - 1, height, LANES), s16),
            pltpu.VMEM((chunks, chips - 1, height, LANES), s16),
            pltpu.VMEM((near, part, height, LANES), s16),
            pltpu.VMEM((near, 2, part, height, LANES), s16),
            pltpu.VMEM((py_count, 2, 16, width), f32),
            pltpu.VMEM((2, NY, width), bf16),
        ]
        + [pltpu.VMEM((NX, NX), bf16)] * 4
        + [
            pltpu.VMEM((chips, 2, near, 2 * ky_part + 8, width), s16),
            pltpu.VMEM((chips, 2, near, 2 * ky_part + 8, width), s16),
            pltpu.VMEM((8 * ky_part, NX), bf16),
            pltpu.VMEM((4 * near * ky_part, width), f32),
            pltpu.VMEM((8, LANES), f32),
            pltpu.VMEM((chips, 2, near, 8, LANES), f32),
            dma((chunks, chips)),
            dma((chunks, chips)),
            dma((chunks, chips - 1)),
            dma((chunks, chips - 1)),
            dma((near, 2, part)),
            dma((near, 2, part)),
            dma((chips, 2, near)),
            dma((chips, 2, near)),
            dma((chips, 2, near)),
            dma((chips, 2, near)),
        ],
        compiler_params=pltpu.CompilerParams(
            collective_id=0, has_side_effects=True, vmem_limit_bytes=EXCHANGE_VMEM * 1024 * 1024
        ),
        name="exchange",
    )(grid, counts, *tables)


def local(cell_ids, offset_x, offset_y, mass, live, tile_owner, counts):
    px_count = lax.axis_size("px")
    py_count = lax.axis_size("py")
    row_count = NX // px_count
    col_count = NY // py_count
    parts = px_count // PLANES
    devices = px_count * py_count
    ky_part = NY // devices
    grid = spread(
        cell_ids[0], tile_owner, offset_x[0], offset_y[0], mass[0], live[0], row_count, col_count,
        px_count * PLANES,
    )
    bucket_count = counts.shape[-1]
    lane_tiles = NX // LANES
    if px_count == PLANES and py_count % 2 == 0 and lane_tiles % py_count == 0 and bucket_count <= LANES:
        out, begin, factor = exchange(grid, counts[0], dft_parts(), px_count, py_count)
        return (out.reshape(2, PLANES, ky_part, NX) * factor, begin)
    grid = grid.transpose(0, 2, 1, 3).reshape(PLANES, col_count + 16, NX)
    height = col_count + 16
    width = NX // parts
    if parts > 1:
        grid = grid.reshape(PLANES, height, parts, width).transpose(0, 2, 1, 3)
    grid = grid.reshape(px_count // 2, 2, height, width)
    side = lax.axis_index("px") % 2
    keep = lax.dynamic_index_in_dim(grid, side, 1, keepdims=False)
    away = lax.dynamic_index_in_dim(grid, 1 - side, 1, keepdims=False)
    pairs = [(source, source ^ 1) for source in range(px_count)]
    summed = keep + lax.ppermute(away, "px", pairs)
    groups = [list(range(k, px_count, 2)) for k in range(2)]
    got = lax.all_to_all(
        coded_rows(summed, col_count + 8), "px", 0, 0, axis_index_groups=groups, tiled=True
    )
    mine = jnp.sum(plain_rows(got, col_count + 8), axis=0)
    total = jnp.sum(mine)
    by_cols = lax.all_to_all(
        coded_rows(mine, col_count + 8), "py", split_axis=1, concat_axis=0, tiled=True
    )
    part = width // py_count
    ext = plain_rows(by_cols.reshape(py_count, height, part), col_count + 8)
    core = ext[:, :col_count]
    right = jnp.roll(ext[:, col_count : col_count + 4], 1, axis=0)
    left = jnp.roll(ext[:, col_count + 12 :], -1, axis=0)
    core = core + jnp.concatenate(
        [right, jnp.zeros((py_count, col_count - 8, part), jnp.float32), left], axis=1
    )
    data = core.reshape(NY, part)
    cos_hi, cos_lo, sin_hi, sin_lo = dft_tables()
    hi, lo = split(data)
    both = jnp.concatenate([hi, lo], axis=1)
    real = dot(cos_hi, both)
    real = real[:, :part] + real[:, part:] + dot(cos_lo, hi)
    imag = dot(sin_hi, both)
    imag = -(imag[:, :part] + imag[:, part:] + dot(sin_lo, hi))
    lines = jnp.stack([real.reshape(devices, ky_part, part), imag.reshape(devices, ky_part, part)], 1)
    lines = lines.reshape(devices, 2 * ky_part, part)
    power = power_of(jnp.max(jnp.abs(lines), axis=1, keepdims=True))
    coded = coded_as(lines, power)
    count_rows = -(-bucket_count // part)
    spare = -(2 + count_rows) % 8
    side_rows = jnp.concatenate(
        [
            digits(total, part),
            jnp.pad(counts.reshape(-1), (0, count_rows * part - bucket_count)).reshape(-1, part),
            jnp.zeros((spare, part), jnp.int32),
        ]
    ).astype(jnp.int16)
    side_rows = jnp.broadcast_to(side_rows[None], (devices,) + side_rows.shape)
    coded = jnp.concatenate([coded, power.astype(jnp.int16), side_rows], axis=1)
    got = lax.all_to_all(coded, ("px", "py"), split_axis=0, concat_axis=0, tiled=True)
    after = got[:, 2 * ky_part :].astype(jnp.int32)
    lines = got[:, : 2 * ky_part].astype(jnp.float32) * scale_of(after[:, :1])
    total = jnp.sum(number(after[:, 1]))
    column = after[:, 2 : 2 + count_rows].reshape(px_count, py_count, 1, count_rows * part)
    column = lax.dynamic_index_in_dim(column, lax.axis_index("py"), 1, keepdims=False)
    column = column[:, :, :bucket_count][:, None]
    got = lines.reshape(PLANES, parts * py_count, 2, ky_part, part).transpose(2, 0, 3, 1, 4)
    got = got.reshape(2 * PLANES * ky_part, NX)
    hi, lo = split(got)
    rows = PLANES * ky_part
    both = jnp.concatenate([hi, lo], axis=0)
    by_cos = dot(both, cos_hi)
    by_cos = by_cos[: 2 * rows] + by_cos[2 * rows :] + dot(hi, cos_lo)
    by_sin = dot(both, sin_hi)
    by_sin = by_sin[: 2 * rows] + by_sin[2 * rows :] + dot(hi, sin_lo)
    out = jnp.stack([by_cos[:rows] + by_sin[rows:], by_cos[rows:] - by_sin[:rows]])
    out = out.reshape(2, PLANES, ky_part, NX)
    spectrum = scaled(out, total)
    column_sum = jnp.sum(column, axis=0)
    reached = lax.broadcasted_iota(jnp.int32, column.shape, 0) < lax.axis_index("px")
    earlier = jnp.sum(jnp.where(reached, column, 0), axis=0)
    preceding = jnp.cumsum(column_sum, axis=-1) - column_sum
    bucket_start = (preceding + earlier).astype(jnp.int32)
    return (spectrum, bucket_start)


def solution(mesh):
    placed = (
        P("px", "py", None),
        P("px", "py", None),
        P("px", "py", None),
        P("px", "py", None),
        P("px", "py", None),
        P("px", "py"),
        P("px", "py", None),
    )
    return jax.shard_map(
        local,
        mesh=mesh,
        in_specs=placed,
        out_specs=(P(None, None, ("px", "py"), None), P("px", "py", None)),
        check_vma=False,
    )
```
